256 devices in a mesh: seq: 32 (over z_lo, x, core), res: 8 (over z_hi, y).
Axes of the slice: x: 4, y: 4, z: 8 (z_hi: 2, z_lo: 4; z = z_hi * 4 + z_lo), core: 2. Of those that a mesh axis runs over, the one named last changes fastest.
Arguments:
- embedded_aligned_rows: bfloat16 [96, 1024, 768], P('seq', 'res'), may hold values from -12 to 12
- norm_multiplier: float32 [768], replicated, may hold values from 0.1 to 1.9
- asker_projector: bfloat16 [768, 768], replicated, may hold values from -1 to 1
- matcher_projector: bfloat16 [768, 768], replicated, may hold values from -1 to 1
- content_projector: bfloat16 [768, 768], replicated, may hold values from -0.21875 to 0.21875
- final_projector: bfloat16 [768, 768], replicated, may hold values from -0.21875 to 0.21875
Outputs:
- mixed: bfloat16 [96, 1024, 768], P('seq', 'res')
The draws below stay inside these ranges and needn't reach their ends.
All inputs are finite; a program needn't handle non-finite values.
Results may differ from the reference program's by a relative error of at most 0.01.
Values may be sent and summed in bfloat16 or wider, within the bound.
A program may use at most 64 MiB of HBM per device.

```python
import jax
import jax.numpy as jnp
from jax import lax

D = 768
HEADS = 12
SEQS = 96
RES = 1024
N_SEQ = 32


def weight_pair(key):
    base = jax.random.normal(jax.random.fold_in(key, 21), (D, D), jnp.float32) / jnp.sqrt(jnp.float32(D))
    other = jax.random.normal(jax.random.fold_in(key, 22), (D, D), jnp.float32) / jnp.sqrt(jnp.float32(D))
    return (base, other)


def draw_asker_projector(key, part):
    base, other = weight_pair(key)
    return jnp.clip(base, -1.0, 1.0).astype(jnp.bfloat16)


def draw_matcher_projector(key, part):
    base, other = weight_pair(key)
    content_array = other
    return jnp.clip(content_array, -1.0, 1.0).astype(jnp.bfloat16)


def draw_embedded_aligned_rows(key, part):
    noise = jax.random.normal(jax.random.fold_in(key, 11), (SEQS, RES, D), jnp.float32)
    content_array = noise
    return jnp.clip(content_array, -12.0, 12.0).astype(jnp.bfloat16)


def scatter_about(rng, extent, scale, most, kind=jnp.bfloat16):
    return jnp.clip(scale * jax.random.normal(rng, extent, jnp.float32), -most, most).astype(kind)


def setup_inputs(seed: int = 0) -> dict:
    streams_of = jax.random.split(jax.random.key(seed), 7)
    return {
        "embedded_aligned_rows": draw_embedded_aligned_rows(jax.random.fold_in(streams_of[6], 71), 0),
        "norm_multiplier": jnp.clip(1.0 + 0.18 * jax.random.normal(streams_of[1], (D,), jnp.float32), 0.1, 1.9),
        "asker_projector": draw_asker_projector(jax.random.fold_in(streams_of[6], 71), 0),
        "matcher_projector": draw_matcher_projector(jax.random.fold_in(streams_of[6], 71), 0),
        "content_projector": scatter_about(streams_of[4], (D, D), D ** -0.5, 0.21875),
        "final_projector": scatter_about(streams_of[5], (D, D), D ** -0.5, 0.21875),
    }


def standardize_rows(embedded_aligned_rows, norm_multiplier):
    content_array = embedded_aligned_rows.astype(jnp.float32)
    center = content_array - lax.optimization_barrier(jnp.mean(content_array, axis=-1, keepdims=True))
    spread = lax.optimization_barrier(jnp.mean(center * center, axis=-1, keepdims=True))
    return (center / jnp.sqrt(spread + 1e-05) * norm_multiplier).astype(jnp.bfloat16)

def reference(embedded_aligned_rows, norm_multiplier, asker_projector, matcher_projector, content_projector, final_projector):
    element_number, overall_span, embedding_dimension = embedded_aligned_rows.shape
    heads = HEADS
    hsize = embedding_dimension // heads
    tile_group = embedded_aligned_rows.reshape(N_SEQ, element_number // N_SEQ, overall_span, embedding_dimension)
    scale = 1.0 / (jnp.sqrt(jnp.float32(hsize)) * jnp.sqrt(jnp.float32(element_number)))

    def project(normed, weight):
        rows = normed.reshape(-1, embedding_dimension)
        out = jnp.dot(rows, weight, preferred_element_type=jnp.float32).astype(jnp.bfloat16)
        return out.reshape(normed.shape[0], overall_span, heads, hsize)

    def add_logits(total, block):
        normed = standardize_rows(block, norm_multiplier)
        query = project(normed, asker_projector).astype(jnp.float32)
        keys = project(normed, matcher_projector).astype(jnp.float32)
        return (total + jnp.einsum('sihe,sjhe->hij', query, keys), None)
    start = jnp.zeros((heads, overall_span, overall_span), jnp.float32)
    logits, _ = lax.scan(add_logits, start, tile_group)
    probs = jax.nn.softmax(logits * scale, axis=-1).astype(jnp.bfloat16)
    weights = probs.astype(jnp.float32)

    def mix_block(carry, block):
        normed = standardize_rows(block, norm_multiplier)
        value = project(normed, content_projector).astype(jnp.float32)
        attended = jnp.einsum('hij,sjhe->sihe', weights, value).astype(jnp.bfloat16)
        rows = attended.reshape(-1, embedding_dimension)
        mixed = jnp.dot(rows, final_projector, preferred_element_type=jnp.float32).astype(jnp.bfloat16)
        return (carry, mixed.reshape(block.shape))
    _, mixed = lax.scan(mix_block, jnp.zeros((), jnp.float32), tile_group)
    return mixed.reshape(element_number, overall_span, embedding_dimension)
```

```python
import functools

import jax
import jax.numpy as jnp
from jax import lax
from jax.experimental import pallas as pl
from jax.experimental.pallas import tpu as pltpu
from jax.sharding import PartitionSpec as P

MESH = pl.DeviceIdType.MESH
BF = jnp.bfloat16
F32 = jnp.float32
NX, NY, NZ = 4, 4, 4
S, B, D = 3, 128, 768
H, E = 3, 64
ROWS = 256
HALF = NY * B


def kernel(
    x_hbm, gain_ref, wq_hbm, wk_hbm, wv_hbm, wf_hbm, out_ref,
    xo, xp, xn, wq, wk, wv, wf, qt, kt, vt, qr, kr, vr, qn, xs, xr, zs, zr, pf, os, orr,
    lsem, zss, zrs, qss, qrs, kss, krs, vss, vrs, kfs, kfr, vfs, vfr,
    xss, xrs, lss, lrs, pzs, pzr, pxs, pxr, oss, osr,
):
    seq, res = lax.axis_index("seq"), lax.axis_index("res")
    c, x, zl = lax.rem(seq, 2), lax.rem(seq // 2, NX), seq // (2 * NX)
    y, zh = lax.rem(res, NY), res // NY

    def dev(x=x, zl=zl, c=c, y=y, zh=zh):
        return ((zl * NX + x) * 2 + c, zh * NY + y)

    def up(i, d, n):
        return lax.rem(i + d, n)

    other = dev(c=1 - c)

    def send(src, dst, ss, rs, to):
        return pltpu.make_async_remote_copy(
            src_ref=src, dst_ref=dst, send_sem=ss, recv_sem=rs, device_id=to, device_id_type=MESH
        )

    loads = [
        pltpu.make_async_copy(a, b, lsem.at[i])
        for i, (a, b) in enumerate(((x_hbm, xo), (wq_hbm, wq), (wk_hbm, wk), (wv_hbm, wv), (wf_hbm, wf)))
    ]
    for copy in loads:
        copy.start()

    barrier = pltpu.get_barrier_semaphore()
    peers = [other, dev(zh=1 - zh)]
    peers += [dev(x=up(x, d, NX)) for d in range(1, NX)]
    peers += [dev(zl=up(zl, d, NZ)) for d in range(1, NZ)]
    peers += [dev(y=up(y, d, NY), c=k) for d in range(1, NY) for k in range(2)]
    for peer in peers:
        pl.semaphore_signal(barrier, inc=1, device_id=peer, device_id_type=MESH)
    pl.semaphore_wait(barrier, len(peers))

    loads[0].wait()

    def rows_over(s):
        return send(xo.at[s], xp.at[s], zss.at[s], zrs.at[s], dev(zh=1 - zh))

    for s in range(S):
        rows_over(s).start()

    def norm(rows):
        rows = rows.astype(F32)
        center = rows - jnp.mean(rows, axis=-1, keepdims=True)
        spread = jnp.mean(center * center, axis=-1, keepdims=True)
        return (center * lax.rsqrt(spread + 1e-05) * gain_ref[...]).astype(BF)

    def project(normed, w):
        out = jnp.dot(normed, w[...], preferred_element_type=F32).astype(BF)
        return out.T.reshape(NY, H, E, B)

    def q_copy(s, d):
        b = (-d) % NY
        to = dev(y=up(y, d, NY), c=b // 2)
        return send(qt.at[up(y, d, NY), s], qr.at[b % 2, c, s], qss.at[d, s], qrs.at[b % 2, c, s], to)

    def kv_copy(t, r, ss, rs, half, s, d):
        g = up(y, d, NY)
        return send(
            t.at[half, g, s], r.at[half, (-d) % NY, c, s], ss.at[half, d - 1, s], rs.at[half, d - 1, s], dev(y=g)
        )

    def forward(r, ss, rs, half, rel):
        part = r.at[half, rel, c]
        return send(part, part, ss.at[half, rel], rs.at[half, rel], other)

    k_copy = functools.partial(kv_copy, kt, kr, kss, krs)
    v_copy = functools.partial(kv_copy, vt, vr, vss, vrs)
    k_forward = functools.partial(forward, kr, kfs, kfr)
    v_forward = functools.partial(forward, vr, vfs, vfr)

    for copy in loads[1:3]:
        copy.wait()

    @pl.loop(0, S)
    def _(s):
        normed = norm(xo[s])
        xn[s] = normed
        qt[:, s] = project(normed, wq)
        kt[0, :, s] = project(normed, wk)
        for d in range(1, NY):
            q_copy(s, d).start()

        @pl.when(c == 1)
        def _():
            q_copy(s, 0).start()

        @pl.when(c == 0)
        def _():
            qr[0, 0, s] = qt[y, s]

        for d in range(1, NY):
            k_copy(0, s, d).start()
        kr[0, 0, c, s] = kt[0, y, s]

    k_forward(0, 0).start()
    loads[3].wait()

    @pl.loop(0, S)
    def _(s):
        v = project(xn[s], wv)
        vt[0, :, s] = v
        vr[0, 0, c, s] = vt[0, y, s]

    v_forward(0, 0).start()

    def partner(s):
        rows_over(s).wait_recv()
        normed = norm(xp[s])
        kt[1, :, s] = project(normed, wk)
        for d in range(1, NY):
            k_copy(1, s, d).start()
        kr[1, 0, c, s] = kt[1, y, s]
        vt[1, :, s] = project(normed, wv)
        vr[1, 0, c, s] = vt[1, y, s]

    def forward_all(copy, fwd, half):
        for d in range(1, NY):
            for s in range(S):
                copy(half, s, d).wait_recv()
            fwd(half, (-d) % NY).start()

    def columns(r, half, h):
        return jnp.concatenate(
            [r[half, rel, :, :, h].reshape(2 * S * E, B) for rel in range(NY)], axis=1
        )

    def x_copy(half, d):
        g = up(x, d, NX)
        return send(xs.at[half, g], xr.at[half, d - 1], xss.at[half, d - 1], xrs.at[half, d - 1], dev(x=g))

    def z_copy(half, d):
        g = up(zl, d, NZ)
        return send(zs.at[half, g], zr.at[half, d - 1], lss.at[half, d - 1], lrs.at[half, d - 1], dev(zl=g))

    def logits(half):
        for rel in range(NY):
            k_forward(half, rel).wait_recv()

        @pl.loop(0, H)
        def _(h):
            part = jnp.dot(qn[h], columns(kr, half, h), preferred_element_type=F32).astype(BF)
            xs[half, :, h] = part.reshape(NX, ROWS // NX, HALF)

        for d in range(1, NX):
            x_copy(half, d).start()

    def over_x(half):
        for d in range(1, NX):
            x_copy(half, d).wait_recv()
        for h in range(H):
            total = xs[half, x, h].astype(F32)
            for d in range(1, NX):
                total += xr[half, d - 1, h].astype(F32)
            zs[half, :, h] = total.astype(BF).reshape(NZ, ROWS // NX // NZ, HALF)
        for d in range(1, NZ):
            z_copy(half, d).start()

    def over_z(half):
        for d in range(1, NZ):
            z_copy(half, d).wait_recv()
        total = zs[half, zl].astype(F32)
        for d in range(1, NZ):
            total += zr[half, d - 1].astype(F32)
        return total

    @pl.loop(0, 2)
    def _(s):
        partner(s)

    forward_all(k_copy, k_forward, 0)
    for b, k in ((0, 1), (1, 0), (1, 1)):
        for s in range(S):
            send(qt.at[0, s], qr.at[b, k, s], qss.at[0, s], qrs.at[b, k, s], other).wait_recv()

    @pl.when(c == 1)
    def _():
        for s in range(S):
            send(qt.at[0, s], qr.at[0, 0, s], qss.at[0, s], qrs.at[0, 0, s], other).wait_recv()

    @pl.loop(0, H)
    def _(h):
        cols = [qr[b, :, :, h].reshape(2 * S * E, B).T for b in range(2)]
        qn[h] = jnp.concatenate(cols, axis=0)

    logits(0)
    partner(2)
    k_forward(1, 0).start()
    v_forward(1, 0).start()

    @pl.loop(0, 2)
    def _(half):
        @pl.loop(0, S)
        def _(s):
            for d in range(1, NY):
                v_copy(half, s, d).start()

    over_x(0)
    forward_all(k_copy, k_forward, 1)
    logits(1)
    first = over_z(0)
    over_x(1)
    second = over_z(1)

    scale = 1.0 / (8.0 * (96.0 ** 0.5))
    top = jnp.maximum(jnp.max(first, axis=-1, keepdims=True), jnp.max(second, axis=-1, keepdims=True))
    first = jnp.exp((first - top) * scale)
    second = jnp.exp((second - top) * scale)
    whole = jnp.sum(first, axis=-1, keepdims=True) + jnp.sum(second, axis=-1, keepdims=True)
    inverse = 1.0 / whole
    pf[x, zl, :, :, :HALF] = (first * inverse).astype(BF)
    pf[x, zl, :, :, HALF:] = (second * inverse).astype(BF)

    def pz_copy(d):
        part = pf.at[x, zl]
        return send(part, part, pzs.at[d - 1], pzr.at[d - 1], dev(zl=up(zl, d, NZ)))

    def px_copy(d):
        part = pf.at[x]
        return send(part, part, pxs.at[d - 1], pxr.at[d - 1], dev(x=up(x, d, NX)))

    for d in range(1, NZ):
        pz_copy(d).start()
    for d in range(1, NZ):
        pz_copy(d).wait_recv()
    for d in range(1, NX):
        px_copy(d).start()
    for half in range(2):
        forward_all(v_copy, v_forward, half)
    for half in range(2):
        for rel in range(NY):
            v_forward(half, rel).wait_recv()
    for d in range(1, NX):
        px_copy(d).wait_recv()

    @pl.loop(0, H)
    def _(h):
        weights = pf[:, :, h].reshape(ROWS, 2 * HALF)
        total = jnp.zeros((2 * S * E, ROWS), F32)
        for half in range(2):
            total += lax.dot_general(
                columns(vr, half, h),
                weights[:, half * HALF : (half + 1) * HALF],
                (((1,), (1,)), ((), ())),
                preferred_element_type=F32,
            )
        total = total.astype(BF)
        for b in range(2):
            os[b, :, :, h] = total[:, b * B : (b + 1) * B].reshape(2, S, E, B)

    def o_copy(slot, k):
        b = 2 * c + slot
        return send(os.at[slot, k], orr.at[y], oss.at[slot, k], osr.at[b], dev(y=up(y, b, NY), c=k))

    for slot, k in ((1, 0), (1, 1), (0, 1)):
        o_copy(slot, k).start()

    @pl.when(c == 1)
    def _():
        o_copy(0, 0).start()

    @pl.when(c == 0)
    def _():
        orr[y] = os[0, 0]

    loads[4].wait()
    for b in range(1, NY):
        send(os.at[0, 0], orr.at[b], oss.at[0, 0], osr.at[b], other).wait_recv()

    @pl.when(c == 1)
    def _():
        send(os.at[0, 0], orr.at[0], oss.at[0, 0], osr.at[0], other).wait_recv()

    @pl.loop(0, S)
    def _(s):
        att = orr[:, s].reshape(D, B).T
        out_ref[s] = jnp.dot(att, wf[...], preferred_element_type=F32).astype(BF)

    for s in range(S):
        rows_over(s).wait_send()
        for d in range(1, NY):
            q_copy(s, d).wait_send()
    for half in range(2):
        for d in range(1, NY):
            for s in range(S):
                k_copy(half, s, d).wait_send()
                v_copy(half, s, d).wait_send()
        for rel in range(NY):
            k_forward(half, rel).wait_send()
            v_forward(half, rel).wait_send()
        for d in range(1, NX):
            x_copy(half, d).wait_send()
        for d in range(1, NZ):
            z_copy(half, d).wait_send()
    for d in range(1, NZ):
        pz_copy(d).wait_send()
    for d in range(1, NX):
        px_copy(d).wait_send()
    for slot, k in ((1, 0), (1, 1), (0, 1)):
        o_copy(slot, k).wait_send()

    @pl.when(c == 1)
    def _():
        o_copy(0, 0).wait_send()
        for s in range(S):
            q_copy(s, 0).wait_send()


def body(rows, gain, wq, wk, wv, wf):
    slab = (S, H, E, B)
    dma = pltpu.SemaphoreType.DMA
    scratch = [
        pltpu.VMEM((S, B, D), BF), pltpu.VMEM((S, B, D), BF), pltpu.VMEM((S, B, D), BF),
        pltpu.VMEM((D, D), BF), pltpu.VMEM((D, D), BF), pltpu.VMEM((D, D), BF), pltpu.VMEM((D, D), BF),
        pltpu.VMEM((NY,) + slab, BF), pltpu.VMEM((2, NY) + slab, BF), pltpu.VMEM((2, NY) + slab, BF),
        pltpu.VMEM((2, 2) + slab, BF), pltpu.VMEM((2, NY, 2) + slab, BF), pltpu.VMEM((2, NY, 2) + slab, BF),
        pltpu.VMEM((H, ROWS, 2 * S * E), BF),
        pltpu.VMEM((2, NX, H, ROWS // NX, HALF), BF), pltpu.VMEM((2, NX - 1, H, ROWS // NX, HALF), BF),
        pltpu.VMEM((2, NZ, H, ROWS // NX // NZ, HALF), BF), pltpu.VMEM((2, NZ - 1, H, ROWS // NX // NZ, HALF), BF),
        pltpu.VMEM((NX, NZ, H, ROWS // NX // NZ, 2 * HALF), BF),
        pltpu.VMEM((2, 2) + slab, BF), pltpu.VMEM((NY,) + slab, BF),
        dma((5,)), dma((S,)), dma((S,)),
        dma((NY, S)), dma((2, 2, S)),
        dma((2, NY - 1, S)), dma((2, NY - 1, S)), dma((2, NY - 1, S)), dma((2, NY - 1, S)),
        dma((2, NY)), dma((2, NY)), dma((2, NY)), dma((2, NY)),
        dma((2, NX - 1)), dma((2, NX - 1)), dma((2, NZ - 1)), dma((2, NZ - 1)),
        dma((NZ - 1,)), dma((NZ - 1,)), dma((NX - 1,)), dma((NX - 1,)),
        dma((2, 2)), dma((NY,)),
    ]
    anywhere = pl.BlockSpec(memory_space=pl.ANY)
    vmem = pl.BlockSpec(memory_space=pltpu.VMEM)
    return pl.pallas_call(
        kernel,
        out_shape=jax.ShapeDtypeStruct((S, B, D), BF),
        in_specs=[anywhere, vmem, anywhere, anywhere, anywhere, anywhere],
        out_specs=vmem,
        scratch_shapes=scratch,
        compiler_params=pltpu.CompilerParams(
            collective_id=0, has_side_effects=True, vmem_limit_bytes=56 * 1024 * 1024
        ),
        name="tied_row_attention",
    )(rows, gain.reshape(1, D), wq, wk, wv, wf)


def solution(mesh):
    placed = (P("seq", "res", None), P(), P(), P(), P(), P())
    return jax.shard_map(
        body, mesh=mesh, in_specs=placed, out_specs=P("seq", "res", None), check_vma=False
    )
```

```python
import functools

import jax
import jax.numpy as jnp
from jax import lax
from jax.experimental import pallas as pl
from jax.experimental.pallas import tpu as pltpu
from jax.sharding import PartitionSpec as P

MESH = pl.DeviceIdType.MESH
BF = jnp.bfloat16
F32 = jnp.float32
NX, NY, NZ = 4, 4, 4
S, B, D = 3, 128, 768
H, E = 3, 64
ROWS = 256
HALF = NY * B
SHARE = ROWS // NX // NZ


def kernel(
    x_hbm, gain_ref, wq_hbm, wk_hbm, wv_hbm, out_ref,
    xo, xp, xn, wq, wk, wv, qt, kt, vt, qr, kr, vr, qn, xs, xr, zs, zr, pf, ff, os, orr,
    lsem, zss, zrs, qss, qrs, kss, krs, vss, vrs, kfs, kfr, vfs, vfr,
    xss, xrs, lss, lrs, pzs, pzr, pxs, pxr, fzs, fzr, fxs, fxr, oss, osr,
):
    seq, res = lax.axis_index("seq"), lax.axis_index("res")
    c, x, zl = lax.rem(seq, 2), lax.rem(seq // 2, NX), seq // (2 * NX)
    y, zh = lax.rem(res, NY), res // NY

    def dev(x=x, zl=zl, c=c, y=y, zh=zh):
        return ((zl * NX + x) * 2 + c, zh * NY + y)

    def up(i, d, n):
        return lax.rem(i + d, n)

    other = dev(c=1 - c)

    def send(src, dst, ss, rs, to):
        return pltpu.make_async_remote_copy(
            src_ref=src, dst_ref=dst, send_sem=ss, recv_sem=rs, device_id=to, device_id_type=MESH
        )

    loads = [
        pltpu.make_async_copy(a, b, lsem.at[i])
        for i, (a, b) in enumerate(((x_hbm, xo), (wq_hbm, wq), (wk_hbm, wk), (wv_hbm, wv)))
    ]
    for copy in loads:
        copy.start()

    barrier = pltpu.get_barrier_semaphore()
    peers = [other, dev(zh=1 - zh)]
    peers += [dev(x=up(x, d, NX)) for d in range(1, NX)]
    peers += [dev(zl=up(zl, d, NZ)) for d in range(1, NZ)]
    peers += [dev(y=up(y, d, NY), c=k) for d in range(1, NY) for k in range(2)]
    for peer in peers:
        pl.semaphore_signal(barrier, inc=1, device_id=peer, device_id_type=MESH)
    pl.semaphore_wait(barrier, len(peers))

    loads[0].wait()

    def rows_over(s):
        return send(xo.at[s], xp.at[s], zss.at[s], zrs.at[s], dev(zh=1 - zh))

    for s in range(S):
        rows_over(s).start()

    def norm(rows):
        rows = rows.astype(F32)
        center = rows - jnp.mean(rows, axis=-1, keepdims=True)
        spread = jnp.mean(center * center, axis=-1, keepdims=True)
        return (center * lax.rsqrt(spread + 1e-05) * gain_ref[...].reshape(1, D)).astype(BF)

    def project(normed, w):
        out = jnp.dot(normed, w[...], preferred_element_type=F32).astype(BF)
        return out.T.reshape(NY, H, E, B)

    def q_copy(s, d):
        b = (-d) % NY
        to = dev(y=up(y, d, NY), c=b // 2)
        return send(qt.at[up(y, d, NY), s], qr.at[b % 2, c, s], qss.at[d, s], qrs.at[b % 2, c, s], to)

    def kv_copy(t, r, ss, rs, half, s, d):
        g = up(y, d, NY)
        return send(
            t.at[half, g, s], r.at[half, (-d) % NY, c, s], ss.at[half, d - 1, s], rs.at[half, d - 1, s], dev(y=g)
        )

    def forward(r, ss, rs, half, rel):
        part = r.at[half, rel, c]
        return send(part, part, ss.at[half, rel], rs.at[half, rel], other)

    k_copy = functools.partial(kv_copy, kt, kr, kss, krs)
    v_copy = functools.partial(kv_copy, vt, vr, vss, vrs)
    k_forward = functools.partial(forward, kr, kfs, kfr)
    v_forward = functools.partial(forward, vr, vfs, vfr)

    for copy in loads[1:3]:
        copy.wait()

    @pl.loop(0, S)
    def _(s):
        normed = norm(xo[s])
        xn[s] = normed
        qt[:, s] = project(normed, wq)
        kt[0, :, s] = project(normed, wk)
        for d in range(1, NY):
            q_copy(s, d).start()

        @pl.when(c == 1)
        def _():
            q_copy(s, 0).start()

        @pl.when(c == 0)
        def _():
            qr[0, 0, s] = qt[y, s]

        for d in range(1, NY):
            k_copy(0, s, d).start()
        kr[0, 0, c, s] = kt[0, y, s]

    k_forward(0, 0).start()
    loads[3].wait()

    @pl.loop(0, S)
    def _(s):
        v = project(xn[s], wv)
        vt[0, :, s] = v
        vr[0, 0, c, s] = vt[0, y, s]

    v_forward(0, 0).start()

    def partner(s):
        rows_over(s).wait_recv()
        normed = norm(xp[s])
        kt[1, :, s] = project(normed, wk)
        for d in range(1, NY):
            k_copy(1, s, d).start()
        kr[1, 0, c, s] = kt[1, y, s]
        vt[1, :, s] = project(normed, wv)
        vr[1, 0, c, s] = vt[1, y, s]

    def forward_all(copy, fwd, half):
        for d in range(1, NY):
            for s in range(S):
                copy(half, s, d).wait_recv()
            fwd(half, (-d) % NY).start()

    def columns(r, half, h):
        return jnp.concatenate(
            [r[half, rel, :, :, h].reshape(2 * S * E, B) for rel in range(NY)], axis=1
        )

    def x_copy(half, h, d):
        g = up(x, d, NX)
        at = (half, h, d - 1)
        return send(xs.at[half, h, g], xr.at[at], xss.at[at], xrs.at[at], dev(x=g))

    def z_copy(half, h, d):
        g = up(zl, d, NZ)
        at = (half, h, d - 1)
        return send(zs.at[half, h, g], zr.at[at], lss.at[at], lrs.at[at], dev(zl=g))

    def pz_copy(half, h, d):
        part, at = pf.at[half, h, x, zl], (half, h, d - 1)
        return send(part, part, pzs.at[at], pzr.at[at], dev(zl=up(zl, d, NZ)))

    def px_copy(half, h, d):
        part, at = pf.at[half, h, x], (half, h, d - 1)
        return send(part, part, pxs.at[at], pxr.at[at], dev(x=up(x, d, NX)))

    def fz_copy(d):
        part = ff.at[x, zl]
        return send(part, part, fzs.at[d - 1], fzr.at[d - 1], dev(zl=up(zl, d, NZ)))

    def fx_copy(d):
        part = ff.at[x]
        return send(part, part, fxs.at[d - 1], fxr.at[d - 1], dev(x=up(x, d, NX)))

    def logits(half):
        for rel in range(NY):
            k_forward(half, rel).wait_recv()

        @pl.loop(0, H)
        def _(h):
            part = jnp.dot(qn[h], columns(kr, half, h), preferred_element_type=F32).astype(BF)
            xs[half, h] = part.reshape(NX, ROWS // NX, HALF)
            for d in range(1, NX):
                x_copy(half, h, d).start()

    def over_x(half, h):
        for d in range(1, NX):
            x_copy(half, h, d).wait_recv()
        total = xs[half, h, x].astype(F32)
        for d in range(1, NX):
            total += xr[half, h, d - 1].astype(F32)
        zs[half, h] = total.astype(BF).reshape(NZ, SHARE, HALF)
        for d in range(1, NZ):
            z_copy(half, h, d).start()

    def over_z(half, h):
        for d in range(1, NZ):
            z_copy(half, h, d).wait_recv()
        total = zs[half, h, zl].astype(F32)
        for d in range(1, NZ):
            total += zr[half, h, d - 1].astype(F32)
        return total

    scale = 1.0 / (8.0 * (96.0**0.5))
    tops, sums, factors = [], [], []

    def near(h):
        total = over_z(0, h)
        top = jnp.max(total, axis=-1, keepdims=True)
        weights = jnp.exp((total - top) * scale)
        tops.append(top)
        sums.append(jnp.sum(weights, axis=-1, keepdims=True))
        pf[0, h, x, zl] = weights.astype(BF)
        for d in range(1, NZ):
            pz_copy(0, h, d).start()

    def far(h):
        total = over_z(1, h)
        top = jnp.maximum(tops[h], jnp.max(total, axis=-1, keepdims=True))
        weights = jnp.exp((total - top) * scale)
        old = jnp.exp((tops[h] - top) * scale)
        inverse = 1.0 / (old * sums[h] + jnp.sum(weights, axis=-1, keepdims=True))
        factors.append(old * inverse)
        pf[1, h, x, zl] = (weights * inverse).astype(BF)
        for d in range(1, NZ):
            pz_copy(1, h, d).start()

    def pass_on(half, h):
        for d in range(1, NZ):
            pz_copy(half, h, d).wait_recv()
        for d in range(1, NX):
            px_copy(half, h, d).start()

    partner(0)
    forward_all(k_copy, k_forward, 0)
    for b, k in ((0, 1), (1, 0), (1, 1)):
        for s in range(S):
            send(qt.at[0, s], qr.at[b, k, s], qss.at[0, s], qrs.at[b, k, s], other).wait_recv()

    @pl.when(c == 1)
    def _():
        for s in range(S):
            send(qt.at[0, s], qr.at[0, 0, s], qss.at[0, s], qrs.at[0, 0, s], other).wait_recv()

    @pl.loop(0, H)
    def _(h):
        cols = [qr[b, :, :, h].reshape(2 * S * E, B).T for b in range(2)]
        qn[h] = jnp.concatenate(cols, axis=0)

    logits(0)
    partner(1)
    over_x(0, 0)
    partner(2)
    k_forward(1, 0).start()
    v_forward(1, 0).start()

    @pl.loop(0, 2)
    def _(half):
        @pl.loop(0, S)
        def _(s):
            for d in range(1, NY):
                v_copy(half, s, d).start()

    over_x(0, 1)
    over_x(0, 2)
    forward_all(k_copy, k_forward, 1)
    logits(1)
    for h in range(H):
        near(h)
    for h in range(H):
        pass_on(0, h)
    over_x(1, 0)
    over_x(1, 1)
    far(0)
    over_x(1, 2)
    far(1)
    forward_all(v_copy, v_forward, 0)
    pass_on(1, 0)
    far(2)
    lane = lax.broadcasted_iota(jnp.int32, (SHARE, B), 1)
    ff[x, zl] = jnp.where(lane == 0, factors[0], jnp.where(lane == 1, factors[1], factors[2]))
    for d in range(1, NZ):
        fz_copy(d).start()
    pass_on(1, 1)
    forward_all(v_copy, v_forward, 1)
    pass_on(1, 2)
    for d in range(1, NZ):
        fz_copy(d).wait_recv()
    for d in range(1, NX):
        fx_copy(d).start()
    for half in range(2):
        for rel in range(NY):
            v_forward(half, rel).wait_recv()

    def o_copy(slot, k, h):
        b = 2 * c + slot
        return send(
            os.at[slot, k, h], orr.at[y, h], oss.at[slot, k, h], osr.at[b, h], dev(y=up(y, b, NY), c=k)
        )

    for d in range(1, NX):
        fx_copy(d).wait_recv()

    @pl.loop(0, H)
    def _(h):
        for half in range(2):
            for d in range(1, NX):
                px_copy(half, h, d).wait_recv()
        factor = jnp.sum(
            jnp.where(lax.broadcasted_iota(jnp.int32, (ROWS, B), 1) == h, ff[...].reshape(ROWS, B), 0.0),
            axis=-1,
            keepdims=True,
        )
        weights = [
            (pf[0, h].reshape(ROWS, HALF).astype(F32) * factor).astype(BF),
            pf[1, h].reshape(ROWS, HALF),
        ]
        total = jnp.zeros((2 * S * E, ROWS), F32)
        for half in range(2):
            total += lax.dot_general(
                columns(vr, half, h),
                weights[half],
                (((1,), (1,)), ((), ())),
                preferred_element_type=F32,
            )
        total = total.astype(BF)
        for b in range(2):
            os[b, :, h] = total[:, b * B : (b + 1) * B].reshape(2, S, E, B)
        for slot, k in ((1, 0), (1, 1), (0, 1)):
            o_copy(slot, k, h).start()

        @pl.when(c == 1)
        def _():
            o_copy(0, 0, h).start()

        @pl.when(c == 0)
        def _():
            orr[y, h] = os[0, 0, h]

    for h in range(H):
        for b in range(1, NY):
            send(os.at[0, 0, h], orr.at[b, h], oss.at[0, 0, h], osr.at[b, h], other).wait_recv()

    @pl.when(c == 1)
    def _():
        for h in range(H):
            send(os.at[0, 0, h], orr.at[0, h], oss.at[0, 0, h], osr.at[0, h], other).wait_recv()

    @pl.loop(0, S)
    def _(s):
        out_ref[s] = orr[:, :, s].reshape(D, B).T

    for s in range(S):
        rows_over(s).wait_send()
        for d in range(1, NY):
            q_copy(s, d).wait_send()
    for half in range(2):
        for d in range(1, NY):
            for s in range(S):
                k_copy(half, s, d).wait_send()
                v_copy(half, s, d).wait_send()
        for rel in range(NY):
            k_forward(half, rel).wait_send()
            v_forward(half, rel).wait_send()
        for h in range(H):
            for d in range(1, NX):
                x_copy(half, h, d).wait_send()
                px_copy(half, h, d).wait_send()
            for d in range(1, NZ):
                z_copy(half, h, d).wait_send()
                pz_copy(half, h, d).wait_send()
    for d in range(1, NZ):
        fz_copy(d).wait_send()
    for d in range(1, NX):
        fx_copy(d).wait_send()
    for h in range(H):
        for slot, k in ((1, 0), (1, 1), (0, 1)):
            o_copy(slot, k, h).wait_send()

    @pl.when(c == 1)
    def _():
        for h in range(H):
            o_copy(0, 0, h).wait_send()
        for s in range(S):
            q_copy(s, 0).wait_send()


def body(rows, gain, wq, wk, wv, wf):
    slab = (S, H, E, B)
    dma = pltpu.SemaphoreType.DMA
    scratch = [
        pltpu.VMEM((S, B, D), BF), pltpu.VMEM((S, B, D), BF), pltpu.VMEM((S, B, D), BF),
        pltpu.VMEM((D, D), BF), pltpu.VMEM((D, D), BF), pltpu.VMEM((D, D), BF),
        pltpu.VMEM((NY,) + slab, BF), pltpu.VMEM((2, NY) + slab, BF), pltpu.VMEM((2, NY) + slab, BF),
        pltpu.VMEM((2, 2) + slab, BF), pltpu.VMEM((2, NY, 2) + slab, BF), pltpu.VMEM((2, NY, 2) + slab, BF),
        pltpu.VMEM((H, ROWS, 2 * S * E), BF),
        pltpu.VMEM((2, H, NX, ROWS // NX, HALF), BF), pltpu.VMEM((2, H, NX - 1, ROWS // NX, HALF), BF),
        pltpu.VMEM((2, H, NZ, SHARE, HALF), BF), pltpu.VMEM((2, H, NZ - 1, SHARE, HALF), BF),
        pltpu.VMEM((2, H, NX, NZ, SHARE, HALF), BF), pltpu.VMEM((NX, NZ, SHARE, B), F32),
        pltpu.VMEM((2, 2, H, S, E, B), BF), pltpu.VMEM((NY, H, S, E, B), BF),
        dma((4,)), dma((S,)), dma((S,)),
        dma((NY, S)), dma((2, 2, S)),
        dma((2, NY - 1, S)), dma((2, NY - 1, S)), dma((2, NY - 1, S)), dma((2, NY - 1, S)),
        dma((2, NY)), dma((2, NY)), dma((2, NY)), dma((2, NY)),
        dma((2, H, NX - 1)), dma((2, H, NX - 1)), dma((2, H, NZ - 1)), dma((2, H, NZ - 1)),
        dma((2, H, NZ - 1)), dma((2, H, NZ - 1)), dma((2, H, NX - 1)), dma((2, H, NX - 1)),
        dma((NZ - 1,)), dma((NZ - 1,)), dma((NX - 1,)), dma((NX - 1,)),
        dma((2, 2, H)), dma((NY, H)),
    ]
    anywhere = pl.BlockSpec(memory_space=pl.ANY)
    vmem = pl.BlockSpec(memory_space=pltpu.VMEM)
    attended = pl.pallas_call(
        kernel,
        out_shape=jax.ShapeDtypeStruct((S, B, D), BF),
        in_specs=[anywhere, vmem, anywhere, anywhere, anywhere],
        out_specs=vmem,
        scratch_shapes=scratch,
        compiler_params=pltpu.CompilerParams(
            collective_id=0, has_side_effects=True, vmem_limit_bytes=56 * 1024 * 1024
        ),
        name="tied_row_attention",
    )(rows, gain, wq, wk, wv)
    mixed = jnp.dot(attended.reshape(S * B, D), wf, preferred_element_type=F32).astype(BF)
    return mixed.reshape(S, B, D)


def solution(mesh):
    placed = (P("seq", "res", None), P(), P(), P(), P(), P())
    return jax.shard_map(
        body, mesh=mesh, in_specs=placed, out_specs=P("seq", "res", None), check_vma=False
    )
```

```python
import functools

import jax
import jax.numpy as jnp
from jax import lax
from jax.experimental import pallas as pl
from jax.experimental.pallas import tpu as pltpu
from jax.sharding import PartitionSpec as P

MESH = pl.DeviceIdType.MESH
BF = jnp.bfloat16
F32 = jnp.float32
NX, NY, NZ = 4, 4, 4
S, B, D = 3, 128, 768
H, E = 3, 64
ROWS = 256
HALF = NY * B
SHARE = ROWS // NX // NZ


def kernel(
    x_hbm, gain_ref, wq_hbm, wk_hbm, wv_hbm, out_ref,
    xo, xp, xn, wq, wk, wv, qt, kt, vt, qr, kr, vr, qn, xs, xr, zs, zr, pf, fz, ff, os, orr,
    lsem, zss, zrs, qss, qrs, kss, krs, vss, vrs, kfs, kfr, vfs, vfr,
    xss, xrs, lss, lrs, pzs, pzr, pxs, pxr, fzs, fzr, fxs, fxr, oss, osr,
):
    seq, res = lax.axis_index("seq"), lax.axis_index("res")
    c, x, zl = lax.rem(seq, 2), lax.rem(seq // 2, NX), seq // (2 * NX)
    y, zh = lax.rem(res, NY), res // NY

    def dev(x=x, zl=zl, c=c, y=y, zh=zh):
        return ((zl * NX + x) * 2 + c, zh * NY + y)

    def up(i, d, n):
        return lax.rem(i + d, n)

    other = dev(c=1 - c)

    def send(src, dst, ss, rs, to):
        return pltpu.make_async_remote_copy(
            src_ref=src, dst_ref=dst, send_sem=ss, recv_sem=rs, device_id=to, device_id_type=MESH
        )

    loads = [
        pltpu.make_async_copy(a, b, lsem.at[i])
        for i, (a, b) in enumerate(((x_hbm, xo), (wq_hbm, wq), (wk_hbm, wk), (wv_hbm, wv)))
    ]
    for copy in loads:
        copy.start()

    barrier = pltpu.get_barrier_semaphore()
    peers = [other, dev(zh=1 - zh)]
    peers += [dev(x=up(x, d, NX)) for d in range(1, NX)]
    peers += [dev(zl=up(zl, d, NZ)) for d in range(1, NZ)]
    peers += [dev(y=up(y, d, NY), c=k) for d in range(1, NY) for k in range(2)]
    for peer in peers:
        pl.semaphore_signal(barrier, inc=1, device_id=peer, device_id_type=MESH)
    pl.semaphore_wait(barrier, len(peers))

    loads[0].wait()

    def landed(ref, rs):
        send(ref, ref, rs, rs, other).wait_recv()

    def left(ref, ss):
        send(ref, ref, ss, ss, other).wait_send()

    def rows_over(s):
        return send(xo.at[s], xp.at[s], zss, zrs.at[s], dev(zh=1 - zh))

    for s in range(S):
        rows_over(s).start()

    def norm(rows):
        rows = rows.astype(F32)
        center = rows - jnp.mean(rows, axis=-1, keepdims=True)
        spread = jnp.mean(center * center, axis=-1, keepdims=True)
        return (center * lax.rsqrt(spread + 1e-05) * gain_ref[...].reshape(1, D)).astype(BF)

    def project(normed, w):
        out = jnp.dot(normed, w[...], preferred_element_type=F32).astype(BF)
        return out.T.reshape(NY, H, E, B)

    def q_copy(s, d):
        b = (-d) % NY
        to = dev(y=up(y, d, NY), c=b // 2)
        return send(qt.at[up(y, d, NY), s], qr.at[b % 2 * 2 + c, s], qss, qrs, to)

    def kv_copy(t, r, ss, rs, half, s, d):
        g = up(y, d, NY)
        return send(t.at[half, g, s], r.at[half, (-d) % NY, c, s], ss, rs.at[half, d - 1], dev(y=g))

    def forward(r, ss, rs, half, rel):
        part = r.at[half, rel, c]
        return send(part, part, ss, rs.at[half], other)

    k_copy = functools.partial(kv_copy, kt, kr, kss, krs)
    v_copy = functools.partial(kv_copy, vt, vr, vss, vrs)
    k_forward = functools.partial(forward, kr, kfs, kfr)
    v_forward = functools.partial(forward, vr, vfs, vfr)

    for copy in loads[1:3]:
        copy.wait()

    @pl.loop(0, S)
    def _(s):
        normed = norm(xo[s])
        xn[s] = normed
        qt[:, s] = project(normed, wq)
        kt[0, :, s] = project(normed, wk)
        for d in range(1, NY):
            q_copy(s, d).start()

        @pl.when(c == 1)
        def _():
            q_copy(s, 0).start()

        @pl.when(c == 0)
        def _():
            qr[0, s] = qt[y, s]

        for d in range(1, NY):
            k_copy(0, s, d).start()
        kr[0, 0, c, s] = kt[0, y, s]

    k_forward(0, 0).start()
    loads[3].wait()

    @pl.loop(0, S)
    def _(s):
        v = project(xn[s], wv)
        vt[0, :, s] = v
        vr[0, 0, c, s] = vt[0, y, s]

    v_forward(0, 0).start()

    def partner(s):
        rows_over(s).wait_recv()
        normed = norm(xp[s])
        kt[1, :, s] = project(normed, wk)
        for d in range(1, NY):
            k_copy(1, s, d).start()
        kr[1, 0, c, s] = kt[1, y, s]
        vt[1, :, s] = project(normed, wv)
        vr[1, 0, c, s] = vt[1, y, s]

    def forward_all(r, rs, fwd, half):
        for d in range(1, NY):
            landed(r.at[half, (-d) % NY, c], rs.at[half, d - 1])
            fwd(half, (-d) % NY).start()

    def columns(r, half, h):
        return jnp.concatenate(
            [r[half, rel, :, :, h].reshape(2 * S * E, B) for rel in range(NY)], axis=1
        )

    def x_copy(half, h, d):
        g = up(x, d, NX)
        return send(xs.at[half, h, g], xr.at[half, h, d - 1], xss, xrs.at[half, h], dev(x=g))

    def z_copy(half, h, d):
        g = up(zl, d, NZ)
        return send(zs.at[half, h, g], zr.at[half, h, d - 1], lss, lrs.at[half, h], dev(zl=g))

    def pz_copy(half, h, d):
        part = pf.at[half, h, x, zl]
        return send(part, part, pzs, pzr.at[half, h], dev(zl=up(zl, d, NZ)))

    def px_copy(half, h, d):
        part = pf.at[half, h, x]
        return send(part, part, pxs, pxr.at[h], dev(x=up(x, d, NX)))

    def fz_copy(h, d):
        part = fz.at[h, zl]
        return send(part, part, fzs, fzr.at[h], dev(zl=up(zl, d, NZ)))

    def fx_copy(h, d):
        part = ff.at[h, x]
        return send(part, part, fxs, fxr.at[h], dev(x=up(x, d, NX)))

    def logits(half):
        landed(kr.at[half, :, c], kfr.at[half])

        @pl.loop(0, H)
        def _(h):
            part = jnp.dot(qn[h], columns(kr, half, h), preferred_element_type=F32).astype(BF)
            xs[half, h] = part.reshape(NX, ROWS // NX, HALF)
            for d in range(1, NX):
                x_copy(half, h, d).start()

    def over_x(half, h):
        landed(xr.at[half, h], xrs.at[half, h])
        total = xs[half, h, x].astype(F32)
        for d in range(1, NX):
            total += xr[half, h, d - 1].astype(F32)
        zs[half, h] = total.astype(BF).reshape(NZ, SHARE, HALF)
        for d in range(1, NZ):
            z_copy(half, h, d).start()

    def over_z(half, h):
        landed(zr.at[half, h], lrs.at[half, h])
        total = zs[half, h, zl].astype(F32)
        for d in range(1, NZ):
            total += zr[half, h, d - 1].astype(F32)
        return total

    scale = 1.0 / (8.0 * (96.0**0.5))
    tops, sums = [], []
    lane = lax.broadcasted_iota(jnp.int32, (SHARE, B), 1)

    def near(h):
        total = over_z(0, h)
        top = jnp.max(total, axis=-1, keepdims=True)
        weights = jnp.exp((total - top) * scale)
        tops.append(top)
        sums.append(jnp.sum(weights, axis=-1, keepdims=True))
        pf[0, h, x, zl] = weights.astype(BF)
        for d in range(1, NZ):
            pz_copy(0, h, d).start()

    def far(h):
        total = over_z(1, h)
        top = jnp.maximum(tops[h], jnp.max(total, axis=-1, keepdims=True))
        weights = jnp.exp((total - top) * scale)
        old = jnp.exp((tops[h] - top) * scale)
        inverse = 1.0 / (old * sums[h] + jnp.sum(weights, axis=-1, keepdims=True))
        fz[h, zl] = jnp.broadcast_to(old * inverse, (SHARE, B))
        pf[1, h, x, zl] = (weights * inverse).astype(BF)
        for d in range(1, NZ):
            fz_copy(h, d).start()
            pz_copy(1, h, d).start()

    def pass_on(half, h):
        if half:
            landed(fz.at[h, pl.ds(0, NZ - 1)], fzr.at[h])
            packed = fz[h, 0]
            for k in range(1, NZ):
                packed = jnp.where(lane == k, fz[h, k], packed)
            ff[h, x] = packed
            for d in range(1, NX):
                fx_copy(h, d).start()
        landed(pf.at[half, h, x, pl.ds(0, NZ - 1)], pzr.at[half, h])
        for d in range(1, NX):
            px_copy(half, h, d).start()

    partner(0)
    forward_all(kr, krs, k_forward, 0)
    @pl.when(c == 0)
    def _():
        landed(qr.at[pl.ds(1, 3)], qrs)

    @pl.when(c == 1)
    def _():
        landed(qr, qrs)

    @pl.loop(0, H)
    def _(h):
        cols = [qr[2 * b : 2 * b + 2, :, h].reshape(2 * S * E, B).T for b in range(2)]
        qn[h] = jnp.concatenate(cols, axis=0)

    logits(0)
    partner(1)
    over_x(0, 0)
    partner(2)
    k_forward(1, 0).start()
    v_forward(1, 0).start()

    @pl.loop(0, 2)
    def _(half):
        @pl.loop(0, S)
        def _(s):
            for d in range(1, NY):
                v_copy(half, s, d).start()

    over_x(0, 1)
    over_x(0, 2)
    forward_all(kr, krs, k_forward, 1)
    logits(1)
    for h in range(H):
        near(h)
    over_x(1, 0)
    for h in range(H):
        pass_on(0, h)
    over_x(1, 1)
    far(0)
    over_x(1, 2)
    far(1)
    forward_all(vr, vrs, v_forward, 0)
    pass_on(1, 0)
    far(2)
    pass_on(1, 1)
    forward_all(vr, vrs, v_forward, 1)
    pass_on(1, 2)
    for half in range(2):
        landed(vr.at[half, :, c], vfr.at[half])

    def o_copy(slot, k, h):
        b = 2 * c + slot
        return send(os.at[slot, k, h], orr.at[y, h], oss, osr, dev(y=up(y, b, NY), c=k))

    @pl.loop(0, H)
    def _(h):
        landed(ff.at[h, pl.ds(0, NX - 1)], fxr.at[h])
        landed(pf.at[:, h, pl.ds(0, NX - 1)], pxr.at[h])
        factor = jnp.concatenate([ff[h, i, :, k : k + 1] for i in range(NX) for k in range(NZ)], axis=0)
        weights = [
            (pf[0, h].reshape(ROWS, HALF).astype(F32) * factor).astype(BF),
            pf[1, h].reshape(ROWS, HALF),
        ]
        total = jnp.zeros((2 * S * E, ROWS), F32)
        for half in range(2):
            total += lax.dot_general(
                columns(vr, half, h),
                weights[half],
                (((1,), (1,)), ((), ())),
                preferred_element_type=F32,
            )
        total = total.astype(BF)
        for b in range(2):
            os[b, :, h] = total[:, b * B : (b + 1) * B].reshape(2, S, E, B)
        for slot, k in ((1, 0), (1, 1), (0, 1)):
            o_copy(slot, k, h).start()

        @pl.when(c == 1)
        def _():
            o_copy(0, 0, h).start()

        @pl.when(c == 0)
        def _():
            orr[y, h] = os[0, 0, h]

    @pl.when(c == 0)
    def _():
        landed(orr.at[pl.ds(1, 3)], osr)

    @pl.when(c == 1)
    def _():
        landed(orr, osr)

    @pl.loop(0, S)
    def _(s):
        out_ref[s] = orr[:, :, s].reshape(D, B).T

    left(xo, zss)
    left(kt.at[:, pl.ds(1, NY - 1)], kss)
    left(vt.at[:, pl.ds(1, NY - 1)], vss)
    left(kr.at[:, :, c], kfs)
    left(vr.at[:, :, c], vfs)
    left(xs.at[:, :, pl.ds(1, NX - 1)], xss)
    left(zs.at[:, :, pl.ds(1, NZ - 1)], lss)
    left(pf.at[:, :, 0, pl.ds(1, NZ - 1)], pzs)
    left(pf.at[:, :, pl.ds(1, NX - 1)], pxs)
    left(fz.at[:, pl.ds(1, NZ - 1)], fzs)
    left(ff.at[:, pl.ds(1, NX - 1)], fxs)

    @pl.when(c == 0)
    def _():
        left(qt.at[pl.ds(1, 3)], qss)
        left(orr.at[pl.ds(1, 3)], oss)

    @pl.when(c == 1)
    def _():
        left(qt, qss)
        left(orr, oss)


def body(rows, gain, wq, wk, wv, wf):
    slab = (S, H, E, B)
    dma = pltpu.SemaphoreType.DMA
    scratch = [
        pltpu.VMEM((S, B, D), BF), pltpu.VMEM((S, B, D), BF), pltpu.VMEM((S, B, D), BF),
        pltpu.VMEM((D, D), BF), pltpu.VMEM((D, D), BF), pltpu.VMEM((D, D), BF),
        pltpu.VMEM((NY,) + slab, BF), pltpu.VMEM((2, NY) + slab, BF), pltpu.VMEM((2, NY) + slab, BF),
        pltpu.VMEM((4,) + slab, BF), pltpu.VMEM((2, NY, 2) + slab, BF), pltpu.VMEM((2, NY, 2) + slab, BF),
        pltpu.VMEM((H, ROWS, 2 * S * E), BF),
        pltpu.VMEM((2, H, NX, ROWS // NX, HALF), BF), pltpu.VMEM((2, H, NX - 1, ROWS // NX, HALF), BF),
        pltpu.VMEM((2, H, NZ, SHARE, HALF), BF), pltpu.VMEM((2, H, NZ - 1, SHARE, HALF), BF),
        pltpu.VMEM((2, H, NX, NZ, SHARE, HALF), BF), pltpu.VMEM((H, NZ, SHARE, B), F32), pltpu.VMEM((H, NX, SHARE, B), F32),
        pltpu.VMEM((2, 2, H, S, E, B), BF), pltpu.VMEM((NY, H, S, E, B), BF),
        dma((4,)), dma, dma((S,)), dma, dma,
        dma, dma((2, NY - 1)), dma, dma((2, NY - 1)), dma, dma((2,)), dma, dma((2,)),
        dma, dma((2, H)), dma, dma((2, H)), dma, dma((2, H)), dma, dma((H,)), dma, dma((H,)), dma, dma((H,)), dma, dma,
    ]
    anywhere = pl.BlockSpec(memory_space=pl.ANY)
    vmem = pl.BlockSpec(memory_space=pltpu.VMEM)
    attended = pl.pallas_call(
        kernel,
        out_shape=jax.ShapeDtypeStruct((S, B, D), BF),
        in_specs=[anywhere, vmem, anywhere, anywhere, anywhere],
        out_specs=vmem,
        scratch_shapes=scratch,
        compiler_params=pltpu.CompilerParams(
            collective_id=0, has_side_effects=True, vmem_limit_bytes=56 * 1024 * 1024
        ),
        name="tied_row_attention",
    )(rows, gain, wq, wk, wv)
    mixed = jnp.dot(attended.reshape(S * B, D), wf, preferred_element_type=F32).astype(BF)
    return mixed.reshape(S, B, D)


def solution(mesh):
    placed = (P("seq", "res", None), P(), P(), P(), P(), P())
    return jax.shard_map(
        body, mesh=mesh, in_specs=placed, out_specs=P("seq", "res", None), check_vma=False
    )
```

```python
import jax
import jax.numpy as jnp
from jax import lax
from jax.experimental import pallas as pl
from jax.experimental.pallas import tpu as pltpu
from jax.sharding import PartitionSpec as P

MESH = pl.DeviceIdType.MESH
BF = jnp.bfloat16
F32 = jnp.float32
NX, NY, NZ = 4, 4, 4
S, B, D = 3, 128, 768
H, E = 3, 64
ROWS = 256
HALF = NY * B
QUARTER = HALF // 2
CHUNKS, CHUNK = 4, B // 4
SHARE = ROWS // NX // NZ


def kernel(
    x_hbm, gain_ref, wq_hbm, wk_hbm, wv_hbm, out_ref,
    xo, xp, xn, wq, wk, wv, wide, qt, kt, vt, kn, qr, kr, vr, kf, qn, qz,
    xs, xr, zs, zr, pf, xsf, xrf, zsf, zrf, pff, fz, ff, os, orr,
    lsem, zss, zrs, qss, qrs, kss, krs, vss, vrs, nss, nrs, kfs, kfr, vfs, vfr, nfs, nfr,
    xss, xrs, lss, lrs, pzs, pzr, pxs, pxr, pnr, fzs, fzr, fxs, fxr, oss, osr,
):
    seq, res = lax.axis_index("seq"), lax.axis_index("res")
    c, x, zl = lax.rem(seq, 2), lax.rem(seq // 2, NX), seq // (2 * NX)
    y, zh = lax.rem(res, NY), res // NY

    def dev(x=x, zl=zl, c=c, y=y, zh=zh):
        return ((zl * NX + x) * 2 + c, zh * NY + y)

    def up(i, d, n):
        return lax.rem(i + d, n)

    other = dev(c=1 - c)

    def send(src, dst, ss, rs, to):
        return pltpu.make_async_remote_copy(
            src_ref=src, dst_ref=dst, send_sem=ss, recv_sem=rs, device_id=to, device_id_type=MESH
        )

    loads = [
        pltpu.make_async_copy(a, b, lsem.at[i])
        for i, (a, b) in enumerate(((x_hbm, xo), (wq_hbm, wq), (wk_hbm, wk), (wv_hbm, wv)))
    ]
    for copy in loads:
        copy.start()

    barrier = pltpu.get_barrier_semaphore()
    peers = [other, dev(zh=1 - zh)]
    peers += [dev(x=up(x, d, NX)) for d in range(1, NX)]
    peers += [dev(zl=up(zl, d, NZ)) for d in range(1, NZ)]
    peers += [dev(y=up(y, d, NY), c=k) for d in range(1, NY) for k in range(2)]
    for peer in peers:
        pl.semaphore_signal(barrier, inc=1, device_id=peer, device_id_type=MESH)
    pl.semaphore_wait(barrier, len(peers))

    loads[0].wait()

    def landed(ref, rs):
        send(ref, ref, rs, rs, other).wait_recv()

    def left(ref, ss):
        send(ref, ref, ss, ss, other).wait_send()

    def rows_over(q):
        rows = pl.ds(q * CHUNK, CHUNK)
        return send(xo.at[:, rows], xp.at[:, rows], zss, zrs.at[q], dev(zh=1 - zh))

    for q in range(CHUNKS):
        rows_over(q).start()

    def norm(rows):
        rows = rows.astype(F32)
        center = rows - jnp.mean(rows, axis=-1, keepdims=True)
        spread = jnp.mean(center * center, axis=-1, keepdims=True)
        return (center * lax.rsqrt(spread + 1e-05) * gain_ref[...].reshape(1, D)).astype(BF)

    def project(normed, w):
        out = jnp.dot(normed, w[...], preferred_element_type=F32).astype(BF)
        return out.T.reshape(NY, H, E, B)

    def q_copy(s, d):
        b = (-d) % NY
        to = dev(y=up(y, d, NY), c=b // 2)
        return send(qt.at[up(y, d, NY), s], qr.at[b % 2 * 2 + c, s], qss, qrs, to)

    def k_copy(s, d):
        g = up(y, d, NY)
        return send(kt.at[g, s], kr.at[(-d) % NY, c, s], kss, krs.at[d - 1], dev(y=g))

    def v_copy(half, s, d):
        g = up(y, d, NY)
        return send(vt.at[half, g, s], vr.at[half, (-d) % NY, c, s], vss, vrs.at[half, d - 1], dev(y=g))

    def far_copy(q, d):
        g = up(y, d, NY)
        return send(kn.at[g, q], kf.at[(-d) % NY, c, q], nss, nrs.at[q // 2, d - 1], dev(y=g))

    def pair(q):
        return pl.ds(2 * q, 2)

    def k_forward(rel):
        part = kr.at[rel, c]
        return send(part, part, kfs, kfr, other)

    def v_forward(half, rel):
        part = vr.at[half, rel, c]
        return send(part, part, vfs, vfr.at[half], other)

    def far_forward(q, rel):
        part = kf.at[rel, c, pair(q)]
        return send(part, part, nfs, nfr.at[q], other)

    for copy in loads[1:3]:
        copy.wait()

    @pl.loop(0, S)
    def _(s):
        normed = norm(xo[s])
        xn[0, s] = normed
        qt[:, s] = project(normed, wq)
        kt[:, s] = project(normed, wk)
        for d in range(1, NY):
            q_copy(s, d).start()

        @pl.when(c == 1)
        def _():
            q_copy(s, 0).start()

        @pl.when(c == 0)
        def _():
            qr[0, s] = qt[y, s]

        for d in range(1, NY):
            k_copy(s, d).start()
        kr[0, c, s] = kt[y, s]

    k_forward(0).start()
    loads[3].wait()

    for g in range(NY):
        wide[:, g * 2 * B : g * 2 * B + H * E] = wk[:, g * H * E : (g + 1) * H * E]
        wide[:, g * 2 * B + H * E : (g + 1) * 2 * B] = jnp.zeros((D, 2 * B - H * E), BF)

    def values(half):
        @pl.loop(0, S)
        def _(s):
            vt[half, :, s] = project(xn[half, s], wv)
            vr[half, 0, c, s] = vt[half, y, s]

        v_forward(half, 0).start()

    values(0)

    def partner(q):
        rows_over(q).wait_recv()
        normed = norm(xp[:, q * CHUNK : (q + 1) * CHUNK].reshape(S * CHUNK, D))
        xn[1, :, q * CHUNK : (q + 1) * CHUNK] = normed.reshape(S, CHUNK, D)
        keys = jnp.dot(normed, wide[...], preferred_element_type=F32).astype(BF).reshape(S, CHUNK, NY * 2 * B)
        for g in range(NY):
            kn[g, q] = keys[:, :, g * 2 * B : (g + 1) * 2 * B]
        for d in range(1, NY):
            far_copy(q, d).start()
        kf[0, c, q] = kn[y, q]

    def columns(r, h):
        return jnp.concatenate([r[rel, :, :, h].reshape(2 * S * E, B) for rel in range(NY)], axis=1)

    def key_rows(part, tile):
        lanes = pl.ds(tile * B, B)
        return jnp.concatenate(
            [
                jnp.concatenate(
                    [kf[rel, i, pair(part), s, :, lanes].reshape(2 * CHUNK, B) for rel in range(NY)], axis=0
                )
                for i in range(2)
                for s in range(S)
            ],
            axis=1,
        )

    def piece(near, far, p):
        return far.at[p - 1] if p else near

    def x_copy(p, h, d):
        g = up(x, d, NX)
        return send(
            piece(xs, xsf, p).at[h, g], piece(xr, xrf, p).at[h, d - 1], xss.at[min(p, 1)], xrs.at[p, h], dev(x=g)
        )

    above, below = up(x, 1, NX), up(x, 3, NX)

    def gather_first(h):
        part = pf.at[h, x]
        return [send(part, part, pxs.at[0], pnr.at[h], dev(x=to)) for to in (above, below)]

    def gather_second(h):
        landed(pf.at[h, pl.ds(0, 2)], pnr.at[h])
        for source, to, first in ((below, above, 0), (above, below, 2)):
            part = pf.at[h, source, pl.ds(first, 2)]
            send(part, part, pxs.at[0], pxr.at[0, h], dev(x=to)).start()

    def z_copy(p, h, d):
        g = up(zl, d, NZ)
        return send(
            piece(zs, zsf, p).at[h, g], piece(zr, zrf, p).at[h, d - 1], lss.at[min(p, 1)], lrs.at[p, h], dev(zl=g)
        )

    def pz_copy(p, h, d):
        part = piece(pf, pff, p).at[h, x, zl]
        return send(part, part, pzs.at[min(p, 1)], pzr.at[p, h], dev(zl=up(zl, d, NZ)))

    def px_copy(p, h, d):
        part = piece(pf, pff, p).at[h, x]
        return send(part, part, pxs.at[min(p, 1)], pxr.at[p, h], dev(x=up(x, d, NX)))

    def fz_copy(d):
        part = fz.at[zl]
        return send(part, part, fzs, fzr, dev(zl=up(zl, d, NZ)))

    def fx_copy(d):
        part = ff.at[x]
        return send(part, part, fxs, fxr, dev(x=up(x, d, NX)))

    def logits(p):
        if p:
            landed(kf.at[:, c, pair(p - 1)], nfr.at[p - 1])
            rows = [key_rows(p - 1, tile) for tile in range(2)]
        else:
            landed(kr.at[:, c], kfr)
        for h in range(H):
            if p:
                part = lax.dot_general(
                    qz[h], rows[h // 2], (((1,), (1,)), ((), ())), preferred_element_type=F32
                ).astype(BF)
                xsf[p - 1, h] = part.reshape(NX, ROWS // NX, QUARTER)
            else:
                part = jnp.dot(qn[h], columns(kr, h), preferred_element_type=F32).astype(BF)
                xs[h] = part.reshape(NX, ROWS // NX, HALF)
            for d in range(1, NX):
                x_copy(p, h, d).start()

    def over_x(p, h):
        mine, theirs, into = piece(xs, xsf, p), piece(xr, xrf, p), piece(zs, zsf, p)
        landed(theirs.at[h], xrs.at[p, h])
        total = mine[h, x].astype(F32)
        for d in range(1, NX):
            total += theirs[h, d - 1].astype(F32)
        into[h] = total.astype(BF).reshape(NZ, SHARE, total.shape[-1])
        for d in range(1, NZ):
            z_copy(p, h, d).start()

    scale = 1.0 / (8.0 * (96.0**0.5))
    tops, sums = [[], []], [[], []]
    lane = lax.broadcasted_iota(jnp.int32, (SHARE, B), 1)
    factors = [jnp.zeros((SHARE, B), F32)]

    def softmax(p, h):
        mine, theirs = piece(zs, zsf, p), piece(zr, zrf, p)
        landed(theirs.at[h], lrs.at[p, h])
        total = mine[h, zl].astype(F32)
        for d in range(1, NZ):
            total += theirs[h, d - 1].astype(F32)
        top = jnp.max(total, axis=-1, keepdims=True)
        if p:
            top = jnp.maximum(top, tops[p - 1][h])
        weights = jnp.exp((total - top) * scale)
        whole = jnp.sum(weights, axis=-1, keepdims=True)
        if p < 2:
            tops[p].append(top)
            sums[p].append(whole)
        else:
            old = [jnp.exp((tops[i][h] - top) * scale) for i in range(2)]
            inverse = 1.0 / (old[0] * sums[0][h] + old[1] * sums[1][h] + whole)
            weights *= inverse
            for i in range(2):
                factors[0] = jnp.where(lane == 4 * i + h, old[i] * inverse, factors[0])
        piece(pf, pff, p)[h, x, zl] = weights.astype(BF)
        for d in range(1, NZ):
            pz_copy(p, h, d).start()

    def pass_on(p, h):
        landed(piece(pf, pff, p).at[h, x, pl.ds(0, NZ - 1)], pzr.at[p, h])
        for copy in [px_copy(p, h, d) for d in range(1, NX)] if p else gather_first(h):
            copy.start()

    def share_keys(part):
        for d in range(1, NY):
            landed(kf.at[(-d) % NY, c, pair(part)], nrs.at[part, d - 1])
            far_forward(part, (-d) % NY).start()

    def share_values(half):
        for d in range(1, NY):
            landed(vr.at[half, (-d) % NY, c], vrs.at[half, d - 1])
            v_forward(half, (-d) % NY).start()

    partner(0)
    for d in range(1, NY):
        landed(kr.at[(-d) % NY, c], krs.at[d - 1])
        k_forward((-d) % NY).start()
    @pl.when(c == 0)
    def _():
        landed(qr.at[pl.ds(1, 3)], qrs)

    @pl.when(c == 1)
    def _():
        landed(qr, qrs)

    @pl.loop(0, H)
    def _(h):
        cols = [qr[2 * b : 2 * b + 2, :, h].reshape(2 * S * E, B).T for b in range(2)]
        qn[h] = jnp.concatenate(cols, axis=0)

    logits(0)
    partner(1)
    far_forward(0, 0).start()
    none = jnp.zeros((E, ROWS), BF)
    for h in range(H):
        rows = []
        for i in range(2):
            for s in range(S):
                query = jnp.concatenate([qr[2 * b + i, s, h] for b in range(2)], axis=1)
                rows += [none, query] if h == 1 else [query, none]
        qz[h] = jnp.concatenate(rows, axis=0).T

    partner(2)
    share_keys(0)
    over_x(0, 0)
    logits(1)
    over_x(0, 1)
    over_x(0, 2)
    partner(3)
    far_forward(1, 0).start()
    values(1)

    @pl.loop(0, 2)
    def _(half):
        @pl.loop(0, S)
        def _(s):
            for d in range(1, NY):
                v_copy(half, s, d).start()

    for h in range(H):
        over_x(1, h)
    share_keys(1)
    for h in range(H):
        softmax(0, h)
    logits(2)
    for h in range(H):
        softmax(1, h)
    over_x(2, 0)
    for h in range(H):
        pass_on(0, h)
    over_x(2, 1)
    over_x(2, 2)
    softmax(2, 0)
    for h in range(H):
        pass_on(1, h)
    softmax(2, 1)
    gather_second(0)
    softmax(2, 2)
    fz[zl] = factors[0]
    for d in range(1, NZ):
        fz_copy(d).start()
    gather_second(1)
    gather_second(2)
    share_values(0)
    share_values(1)
    pass_on(2, 0)
    landed(fz.at[pl.ds(0, NZ - 1)], fzr)
    packed = fz[0]
    for k in range(1, NZ):
        packed = jnp.where((lane >= 8 * k) & (lane < 8 * k + 8), pltpu.roll(fz[k], 8 * k, 1), packed)
    ff[x] = packed
    for d in range(1, NX):
        fx_copy(d).start()
    pass_on(2, 1)
    pass_on(2, 2)
    for half in range(2):
        landed(vr.at[half, :, c], vfr.at[half])

    def o_copy(slot, k, h):
        b = 2 * c + slot
        return send(os.at[slot, k, h], orr.at[y, h], oss, osr, dev(y=up(y, b, NY), c=k))

    landed(ff.at[pl.ds(0, NX - 1)], fxr)
    for h in range(H):
        landed(pf.at[h, 0], pxr.at[0, h])
        for p in (1, 2):
            landed(pff.at[p - 1, h, pl.ds(0, NX - 1)], pxr.at[p, h])
        own = [
            jnp.concatenate(
                [ff[i, :, 8 * k + 4 * n + h : 8 * k + 4 * n + h + 1] for i in range(NX) for k in range(NZ)], axis=0
            )
            for n in range(2)
        ]
        near = (pf[h].reshape(ROWS, HALF).astype(F32) * own[0]).astype(BF)
        first = pff[0, h].reshape(ROWS, QUARTER).astype(F32) * own[1]
        second = pff[1, h].reshape(ROWS, QUARTER).astype(F32)
        low = lax.broadcasted_iota(jnp.int32, (ROWS, B), 1) < B // 2
        far = []
        for k in range(2):
            one, two = first[:, k * B : (k + 1) * B], second[:, k * B : (k + 1) * B]
            far.append(jnp.where(low, one, pltpu.roll(two, B // 2, 1)))
            far.append(jnp.where(low, pltpu.roll(one, B // 2, 1), two))
        far = jnp.concatenate(far, axis=1).astype(BF)
        total = jnp.zeros((2 * S * E, ROWS), F32)
        for half, weights in enumerate((near, far)):
            total += lax.dot_general(
                columns(vr.at[half], h), weights, (((1,), (1,)), ((), ())), preferred_element_type=F32
            )
        total = total.astype(BF)
        for b in range(2):
            os[b, :, h] = total[:, b * B : (b + 1) * B].reshape(2, S, E, B)
        for slot, k in ((1, 0), (1, 1), (0, 1)):
            o_copy(slot, k, h).start()

        @pl.when(c == 1)
        def _():
            o_copy(0, 0, h).start()

        @pl.when(c == 0)
        def _():
            orr[y, h] = os[0, 0, h]

    @pl.when(c == 0)
    def _():
        landed(orr.at[pl.ds(1, 3)], osr)

    @pl.when(c == 1)
    def _():
        landed(orr, osr)

    @pl.loop(0, S)
    def _(s):
        out_ref[s] = orr[:, :, s].reshape(D, B).T

    left(xo, zss)
    left(kt.at[pl.ds(1, NY - 1)], kss)
    left(vt.at[:, pl.ds(1, NY - 1)], vss)
    left(kn.at[pl.ds(1, NY - 1)], nss)
    left(kr.at[:, c], kfs)
    left(vr.at[:, :, c], vfs)
    left(kf.at[:, c], nfs)
    left(xs.at[:, pl.ds(1, NX - 1)], xss.at[0])
    left(xsf.at[:, :, pl.ds(1, NX - 1)], xss.at[1])
    left(zs.at[:, pl.ds(1, NZ - 1)], lss.at[0])
    left(zsf.at[:, :, pl.ds(1, NZ - 1)], lss.at[1])
    left(pf.at[:, 0, pl.ds(1, NZ - 1)], pzs.at[0])
    left(pff.at[:, :, 0, pl.ds(1, NZ - 1)], pzs.at[1])
    left(pf.at[:, pl.ds(1, NX - 1)], pxs.at[0])
    left(pff.at[:, :, pl.ds(1, NX - 1)], pxs.at[1])
    left(fz.at[pl.ds(1, NZ - 1)], fzs)
    left(ff.at[pl.ds(1, NX - 1)], fxs)

    @pl.when(c == 0)
    def _():
        left(qt.at[pl.ds(1, 3)], qss)
        left(orr.at[pl.ds(1, 3)], oss)

    @pl.when(c == 1)
    def _():
        left(qt, qss)
        left(orr, oss)


def body(rows, gain, wq, wk, wv, wf):
    slab = (S, H, E, B)
    dma, vm = pltpu.SemaphoreType.DMA, pltpu.VMEM
    scratch = [
        vm((S, B, D), BF), vm((S, B, D), BF), vm((2, S, B, D), BF),
        vm((D, D), BF), vm((D, D), BF), vm((D, D), BF), vm((D, NY * 2 * B), BF),
        vm((NY,) + slab, BF), vm((NY,) + slab, BF), vm((2, NY) + slab, BF), vm((NY, CHUNKS, S, CHUNK, 2 * B), BF),
        vm((4,) + slab, BF), vm((NY, 2) + slab, BF), vm((2, NY, 2) + slab, BF),
        vm((NY, 2, CHUNKS, S, CHUNK, 2 * B), BF), vm((H, ROWS, 2 * S * E), BF), vm((H, ROWS, 4 * S * E), BF),
        vm((H, NX, ROWS // NX, HALF), BF), vm((H, NX - 1, ROWS // NX, HALF), BF),
        vm((H, NZ, SHARE, HALF), BF), vm((H, NZ - 1, SHARE, HALF), BF), vm((H, NX, NZ, SHARE, HALF), BF),
        vm((2, H, NX, ROWS // NX, QUARTER), BF), vm((2, H, NX - 1, ROWS // NX, QUARTER), BF),
        vm((2, H, NZ, SHARE, QUARTER), BF), vm((2, H, NZ - 1, SHARE, QUARTER), BF),
        vm((2, H, NX, NZ, SHARE, QUARTER), BF),
        vm((NZ, SHARE, B), F32), vm((NX, SHARE, B), F32), vm((2, 2, H, S, E, B), BF), vm((NY, H, S, E, B), BF),
        dma((4,)), dma, dma((CHUNKS,)), dma, dma, dma, dma((NY - 1,)), dma, dma((2, NY - 1)), dma, dma((2, NY - 1)),
        dma, dma, dma, dma((2,)), dma, dma((2,)),
        dma((2,)), dma((3, H)), dma((2,)), dma((3, H)), dma((2,)), dma((3, H)), dma((2,)), dma((3, H)), dma((H,)),
        dma, dma, dma, dma, dma, dma,
    ]
    anywhere = pl.BlockSpec(memory_space=pl.ANY)
    vmem = pl.BlockSpec(memory_space=pltpu.VMEM)
    attended = pl.pallas_call(
        kernel,
        out_shape=jax.ShapeDtypeStruct((S, B, D), BF),
        in_specs=[anywhere, vmem, anywhere, anywhere, anywhere],
        out_specs=vmem,
        scratch_shapes=scratch,
        compiler_params=pltpu.CompilerParams(
            collective_id=0, has_side_effects=True, vmem_limit_bytes=56 * 1024 * 1024
        ),
        name="tied_row_attention",
    )(rows, gain, wq, wk, wv)
    mixed = jnp.dot(attended.reshape(S * B, D), wf, preferred_element_type=F32).astype(BF)
    return mixed.reshape(S, B, D)


def solution(mesh):
    placed = (P("seq", "res", None), P(), P(), P(), P(), P())
    return jax.shard_map(
        body, mesh=mesh, in_specs=placed, out_specs=P("seq", "res", None), check_vma=False
    )
```

```python
import jax
import jax.numpy as jnp
from jax import lax
from jax.experimental import pallas as pl
from jax.experimental.pallas import tpu as pltpu
from jax.sharding import PartitionSpec as P

MESH = pl.DeviceIdType.MESH
BF = jnp.bfloat16
F32 = jnp.float32
NX, NY, NZ = 4, 4, 4
S, B, D = 3, 128, 768
H, E = 3, 64
ROWS = 256
HALF = NY * B
QUARTER = HALF // 2
CHUNKS, CHUNK = 4, B // 4
SHARE = ROWS // NX // NZ


def kernel(
    x_hbm, gain_hbm, wq_hbm, wk_hbm, wv_hbm, out_ref,
    xo, gain_ref, xp, xn, wq, wk, wv, wide, qt, kt, vt, kn, qr, kr, vr, kf, qn, qz,
    xs, xr, zs, zr, pf, xsf, xrf, zsf, zrf, pff, fz, ff, os, orr,
    lsem, zss, zrs, qss, qrs, kss, krs, vss, vrs, nss, nrs, kfs, kfr, vfs, vfr, nfs, nfr,
    xss, xrs, lss, lrs, pzs, pzr, pxs, pxr, pnr, fzs, fzr, fxs, fxr, oss, osr,
):
    seq, res = lax.axis_index("seq"), lax.axis_index("res")
    c, x, zl = lax.rem(seq, 2), lax.rem(seq // 2, NX), seq // (2 * NX)
    y, zh = lax.rem(res, NY), res // NY

    def dev(x=x, zl=zl, c=c, y=y, zh=zh):
        return ((zl * NX + x) * 2 + c, zh * NY + y)

    def up(i, d, n):
        return lax.rem(i + d, n)

    other = dev(c=1 - c)

    def send(src, dst, ss, rs, to):
        return pltpu.make_async_remote_copy(
            src_ref=src, dst_ref=dst, send_sem=ss, recv_sem=rs, device_id=to, device_id_type=MESH
        )

    barrier = pltpu.get_barrier_semaphore()
    peers = [other, dev(zh=1 - zh)]
    peers += [dev(x=up(x, d, NX)) for d in range(1, NX)]
    peers += [dev(zl=up(zl, d, NZ)) for d in range(1, NZ)]
    peers += [dev(y=up(y, d, NY), c=k) for d in range(1, NY) for k in range(2)]
    for peer in peers:
        pl.semaphore_signal(barrier, inc=1, device_id=peer, device_id_type=MESH)
    loads = [
        pltpu.make_async_copy(a, b, lsem.at[i])
        for i, (a, b) in enumerate(((x_hbm, xo), (gain_hbm, gain_ref), (wq_hbm, wq), (wk_hbm, wk), (wv_hbm, wv)))
    ]
    for copy in loads:
        copy.start()

    pl.semaphore_wait(barrier, len(peers))

    loads[0].wait()

    def landed(ref, rs):
        send(ref, ref, rs, rs, other).wait_recv()

    def left(ref, ss):
        send(ref, ref, ss, ss, other).wait_send()

    def rows_over(q):
        rows = pl.ds(q * CHUNK, CHUNK)
        return send(xo.at[:, rows], xp.at[:, rows], zss, zrs.at[q], dev(zh=1 - zh))

    for q in range(CHUNKS):
        rows_over(q).start()

    def norm(rows):
        rows = rows.astype(F32)
        center = rows - jnp.mean(rows, axis=-1, keepdims=True)
        spread = jnp.mean(center * center, axis=-1, keepdims=True)
        return (center * lax.rsqrt(spread + 1e-05) * gain_ref[...].reshape(1, D)).astype(BF)

    def project(normed, w):
        out = jnp.dot(normed, w[...], preferred_element_type=F32).astype(BF)
        return out.T.reshape(NY, H, E, B)

    def q_copy(s, d):
        b = (-d) % NY
        to = dev(y=up(y, d, NY), c=b // 2)
        return send(qt.at[up(y, d, NY), s], qr.at[b % 2 * 2 + c, s], qss, qrs, to)

    def k_copy(s, d):
        g = up(y, d, NY)
        return send(kt.at[g, s], kr.at[(-d) % NY, c, s], kss, krs.at[d - 1], dev(y=g))

    def v_copy(half, s, d):
        g = up(y, d, NY)
        return send(vt.at[half, g, s], vr.at[half, (-d) % NY, c, s], vss, vrs.at[half, d - 1], dev(y=g))

    def far_copy(q, d):
        g = up(y, d, NY)
        return send(kn.at[g, q], kf.at[(-d) % NY, c, q], nss, nrs.at[q // 2, d - 1], dev(y=g))

    def pair(q):
        return pl.ds(2 * q, 2)

    def k_forward(rel):
        part = kr.at[rel, c]
        return send(part, part, kfs, kfr, other)

    def v_forward(half, rel):
        part = vr.at[half, rel, c]
        return send(part, part, vfs, vfr.at[half], other)

    def far_forward(q, rel):
        part = kf.at[rel, c, pair(q)]
        return send(part, part, nfs, nfr.at[q], other)

    for copy in loads[1:4]:
        copy.wait()

    @pl.loop(0, S)
    def _(s):
        normed = norm(xo[s])
        xn[0, s] = normed
        qt[:, s] = project(normed, wq)
        kt[:, s] = project(normed, wk)
        for d in range(1, NY):
            q_copy(s, d).start()

        @pl.when(c == 1)
        def _():
            q_copy(s, 0).start()

        @pl.when(c == 0)
        def _():
            qr[0, s] = qt[y, s]

        for d in range(1, NY):
            k_copy(s, d).start()
        kr[0, c, s] = kt[y, s]

    k_forward(0).start()
    loads[4].wait()

    for g in range(NY):
        wide[:, g * 2 * B : g * 2 * B + H * E] = wk[:, g * H * E : (g + 1) * H * E]
        wide[:, g * 2 * B + H * E : (g + 1) * 2 * B] = jnp.zeros((D, 2 * B - H * E), BF)

    def values(half):
        @pl.loop(0, S)
        def _(s):
            vt[half, :, s] = project(xn[half, s], wv)
            vr[half, 0, c, s] = vt[half, y, s]

        v_forward(half, 0).start()

    values(0)

    def partner(q):
        rows_over(q).wait_recv()
        normed = norm(xp[:, q * CHUNK : (q + 1) * CHUNK].reshape(S * CHUNK, D))
        xn[1, :, q * CHUNK : (q + 1) * CHUNK] = normed.reshape(S, CHUNK, D)
        keys = jnp.dot(normed, wide[...], preferred_element_type=F32).astype(BF).reshape(S, CHUNK, NY * 2 * B)
        for g in range(NY):
            kn[g, q] = keys[:, :, g * 2 * B : (g + 1) * 2 * B]
        for d in range(1, NY):
            far_copy(q, d).start()
        kf[0, c, q] = kn[y, q]

    def columns(r, h):
        return jnp.concatenate([r[rel, :, :, h].reshape(2 * S * E, B) for rel in range(NY)], axis=1)

    def key_rows(part, tile):
        lanes = pl.ds(tile * B, B)
        return jnp.concatenate(
            [
                jnp.concatenate(
                    [kf[rel, i, pair(part), s, :, lanes].reshape(2 * CHUNK, B) for rel in range(NY)], axis=0
                )
                for i in range(2)
                for s in range(S)
            ],
            axis=1,
        )

    def piece(near, far, p):
        return far.at[p - 1] if p else near

    def x_copy(p, h, d):
        g = up(x, d, NX)
        return send(
            piece(xs, xsf, p).at[h, g], piece(xr, xrf, p).at[h, d - 1], xss.at[min(p, 1)], xrs.at[p, h], dev(x=g)
        )

    above, below = up(x, 1, NX), up(x, 3, NX)

    def gather_first(h):
        part = pf.at[h, x]
        return [send(part, part, pxs.at[0], pnr.at[h], dev(x=to)) for to in (above, below)]

    def gather_second(h):
        landed(pf.at[h, pl.ds(0, 2)], pnr.at[h])
        for source, to, first in ((below, above, 0), (above, below, 2)):
            part = pf.at[h, source, pl.ds(first, 2)]
            send(part, part, pxs.at[0], pxr.at[0, h], dev(x=to)).start()

    def z_copy(p, h, d):
        g = up(zl, d, NZ)
        return send(
            piece(zs, zsf, p).at[h, g], piece(zr, zrf, p).at[h, d - 1], lss.at[min(p, 1)], lrs.at[p, h], dev(zl=g)
        )

    def pz_copy(p, h, d):
        part = piece(pf, pff, p).at[h, x, zl]
        return send(part, part, pzs.at[min(p, 1)], pzr.at[p, h], dev(zl=up(zl, d, NZ)))

    def px_copy(p, h, d):
        part = piece(pf, pff, p).at[h, x]
        return send(part, part, pxs.at[min(p, 1)], pxr.at[p, h], dev(x=up(x, d, NX)))

    def fz_copy(d):
        part = fz.at[zl]
        return send(part, part, fzs, fzr, dev(zl=up(zl, d, NZ)))

    def fx_copy(d):
        part = ff.at[x]
        return send(part, part, fxs, fxr, dev(x=up(x, d, NX)))

    def logits(p):
        if p:
            landed(kf.at[:, c, pair(p - 1)], nfr.at[p - 1])
            rows = [key_rows(p - 1, tile) for tile in range(2)]
        else:
            landed(kr.at[:, c], kfr)
        for h in range(H):
            if p:
                part = lax.dot_general(
                    qz[h], rows[h // 2], (((1,), (1,)), ((), ())), preferred_element_type=F32
                ).astype(BF)
                xsf[p - 1, h] = part.reshape(NX, ROWS // NX, QUARTER)
            else:
                part = jnp.dot(qn[h], columns(kr, h), preferred_element_type=F32).astype(BF)
                xs[h] = part.reshape(NX, ROWS // NX, HALF)
            for d in range(1, NX):
                x_copy(p, h, d).start()

    def over_x(p, h):
        mine, theirs, into = piece(xs, xsf, p), piece(xr, xrf, p), piece(zs, zsf, p)
        landed(theirs.at[h], xrs.at[p, h])
        total = mine[h, x].astype(F32)
        for d in range(1, NX):
            total += theirs[h, d - 1].astype(F32)
        into[h] = total.astype(BF).reshape(NZ, SHARE, total.shape[-1])
        for d in range(1, NZ):
            z_copy(p, h, d).start()

    scale = 1.0 / (8.0 * (96.0**0.5))
    tops, sums = [[], []], [[], []]
    lane = lax.broadcasted_iota(jnp.int32, (SHARE, B), 1)
    factors = [jnp.zeros((SHARE, B), F32)]

    def softmax(p, h):
        mine, theirs = piece(zs, zsf, p), piece(zr, zrf, p)
        landed(theirs.at[h], lrs.at[p, h])
        total = mine[h, zl].astype(F32)
        for d in range(1, NZ):
            total += theirs[h, d - 1].astype(F32)
        top = jnp.max(total, axis=-1, keepdims=True)
        if p:
            top = jnp.maximum(top, tops[p - 1][h])
        weights = jnp.exp((total - top) * scale)
        whole = jnp.sum(weights, axis=-1, keepdims=True)
        if p < 2:
            tops[p].append(top)
            sums[p].append(whole)
        else:
            old = [jnp.exp((tops[i][h] - top) * scale) for i in range(2)]
            inverse = 1.0 / (old[0] * sums[0][h] + old[1] * sums[1][h] + whole)
            weights *= inverse
            for i in range(2):
                factors[0] = jnp.where(lane == 4 * i + h, old[i] * inverse, factors[0])
        piece(pf, pff, p)[h, x, zl] = weights.astype(BF)
        for d in range(1, NZ):
            pz_copy(p, h, d).start()

    def pass_on(p, h):
        landed(piece(pf, pff, p).at[h, x, pl.ds(0, NZ - 1)], pzr.at[p, h])
        for copy in [px_copy(p, h, d) for d in range(1, NX)] if p else gather_first(h):
            copy.start()

    def share_keys(part):
        for d in range(1, NY):
            landed(kf.at[(-d) % NY, c, pair(part)], nrs.at[part, d - 1])
            far_forward(part, (-d) % NY).start()

    def share_values(half):
        for d in range(1, NY):
            landed(vr.at[half, (-d) % NY, c], vrs.at[half, d - 1])
            v_forward(half, (-d) % NY).start()

    def send_values(half, s):
        for d in range(1, NY):
            v_copy(half, s, d).start()

    partner(0)
    for s in range(S):
        send_values(0, s)
    for d in range(1, NY):
        landed(kr.at[(-d) % NY, c], krs.at[d - 1])
        k_forward((-d) % NY).start()
    @pl.when(c == 0)
    def _():
        landed(qr.at[pl.ds(1, 3)], qrs)

    @pl.when(c == 1)
    def _():
        landed(qr, qrs)

    @pl.loop(0, H)
    def _(h):
        cols = [qr[2 * b : 2 * b + 2, :, h].reshape(2 * S * E, B).T for b in range(2)]
        qn[h] = jnp.concatenate(cols, axis=0)

    logits(0)
    partner(1)
    far_forward(0, 0).start()
    none = jnp.zeros((E, ROWS), BF)
    for h in range(H):
        rows = []
        for i in range(2):
            for s in range(S):
                query = jnp.concatenate([qr[2 * b + i, s, h] for b in range(2)], axis=1)
                rows += [none, query] if h == 1 else [query, none]
        qz[h] = jnp.concatenate(rows, axis=0).T

    partner(2)
    share_keys(0)
    over_x(0, 0)
    logits(1)
    over_x(0, 1)
    over_x(0, 2)
    partner(3)
    far_forward(1, 0).start()
    values(1)
    over_x(1, 0)
    over_x(1, 1)
    over_x(1, 2)
    share_keys(1)
    softmax(0, 0)
    softmax(0, 1)
    softmax(0, 2)
    logits(2)
    for s in range(S):
        send_values(1, s)
    softmax(1, 0)
    softmax(1, 1)
    softmax(1, 2)
    over_x(2, 0)
    pass_on(0, 0)
    pass_on(0, 1)
    pass_on(0, 2)
    over_x(2, 1)
    over_x(2, 2)
    softmax(2, 0)
    pass_on(1, 0)
    softmax(2, 1)
    gather_second(0)
    softmax(2, 2)
    fz[zl] = factors[0]
    for d in range(1, NZ):
        fz_copy(d).start()
    gather_second(1)
    gather_second(2)
    share_values(0)
    share_values(1)
    pass_on(2, 0)
    pass_on(1, 1)
    landed(fz.at[pl.ds(0, NZ - 1)], fzr)
    packed = fz[0]
    for k in range(1, NZ):
        packed = jnp.where((lane >= 8 * k) & (lane < 8 * k + 8), pltpu.roll(fz[k], 8 * k, 1), packed)
    ff[x] = packed
    for d in range(1, NX):
        fx_copy(d).start()
    pass_on(2, 1)
    pass_on(1, 2)
    pass_on(2, 2)
    for half in range(2):
        landed(vr.at[half, :, c], vfr.at[half])

    def o_copy(slot, k, h):
        b = 2 * c + slot
        return send(os.at[slot, k, h], orr.at[y, h], oss, osr, dev(y=up(y, b, NY), c=k))

    landed(ff.at[pl.ds(0, NX - 1)], fxr)
    for h in range(H):
        own = [
            jnp.concatenate(
                [ff[i, :, 8 * k + 4 * n + h : 8 * k + 4 * n + h + 1] for i in range(NX) for k in range(NZ)], axis=0
            )
            for n in range(2)
        ]
        landed(pf.at[h, 0], pxr.at[0, h])
        near = (pf[h].reshape(ROWS, HALF).astype(F32) * own[0]).astype(BF)
        total = lax.dot_general(
            columns(vr.at[0], h), near, (((1,), (1,)), ((), ())), preferred_element_type=F32
        )
        landed(pff.at[0, h, pl.ds(0, NX - 1)], pxr.at[1, h])
        first = pff[0, h].reshape(ROWS, QUARTER).astype(F32) * own[1]
        landed(pff.at[1, h, pl.ds(0, NX - 1)], pxr.at[2, h])
        second = pff[1, h].reshape(ROWS, QUARTER).astype(F32)
        low = lax.broadcasted_iota(jnp.int32, (ROWS, B), 1) < B // 2
        far = []
        for k in range(2):
            one, two = first[:, k * B : (k + 1) * B], second[:, k * B : (k + 1) * B]
            far.append(jnp.where(low, one, pltpu.roll(two, B // 2, 1)))
            far.append(jnp.where(low, pltpu.roll(one, B // 2, 1), two))
        total += lax.dot_general(
            columns(vr.at[1], h),
            jnp.concatenate(far, axis=1).astype(BF),
            (((1,), (1,)), ((), ())),
            preferred_element_type=F32,
        )
        total = total.astype(BF)
        for b in range(2):
            os[b, :, h] = total[:, b * B : (b + 1) * B].reshape(2, S, E, B)
        for slot, k in ((1, 0), (1, 1), (0, 1)):
            o_copy(slot, k, h).start()

        @pl.when(c == 1)
        def _():
            o_copy(0, 0, h).start()

        @pl.when(c == 0)
        def _():
            orr[y, h] = os[0, 0, h]

    @pl.when(c == 0)
    def _():
        landed(orr.at[pl.ds(1, 3)], osr)

    @pl.when(c == 1)
    def _():
        landed(orr, osr)

    @pl.loop(0, S)
    def _(s):
        out_ref[s] = orr[:, :, s].reshape(D, B).T

    left(xo, zss)
    left(kt.at[pl.ds(1, NY - 1)], kss)
    left(vt.at[:, pl.ds(1, NY - 1)], vss)
    left(kn.at[pl.ds(1, NY - 1)], nss)
    left(kr.at[:, c], kfs)
    left(vr.at[:, :, c], vfs)
    left(kf.at[:, c], nfs)
    left(xs.at[:, pl.ds(1, NX - 1)], xss.at[0])
    left(xsf.at[:, :, pl.ds(1, NX - 1)], xss.at[1])
    left(zs.at[:, pl.ds(1, NZ - 1)], lss.at[0])
    left(zsf.at[:, :, pl.ds(1, NZ - 1)], lss.at[1])
    left(pf.at[:, 0, pl.ds(1, NZ - 1)], pzs.at[0])
    left(pff.at[:, :, 0, pl.ds(1, NZ - 1)], pzs.at[1])
    left(pf.at[:, pl.ds(1, NX - 1)], pxs.at[0])
    left(pff.at[:, :, pl.ds(1, NX - 1)], pxs.at[1])
    left(fz.at[pl.ds(1, NZ - 1)], fzs)
    left(ff.at[pl.ds(1, NX - 1)], fxs)

    @pl.when(c == 0)
    def _():
        left(qt.at[pl.ds(1, 3)], qss)
        left(orr.at[pl.ds(1, 3)], oss)

    @pl.when(c == 1)
    def _():
        left(qt, qss)
        left(orr, oss)


def body(rows, gain, wq, wk, wv, wf):
    slab = (S, H, E, B)
    dma, vm = pltpu.SemaphoreType.DMA, pltpu.VMEM
    scratch = [
        vm((S, B, D), BF), vm((D,), F32), vm((S, B, D), BF), vm((2, S, B, D), BF),
        vm((D, D), BF), vm((D, D), BF), vm((D, D), BF), vm((D, NY * 2 * B), BF),
        vm((NY,) + slab, BF), vm((NY,) + slab, BF), vm((2, NY) + slab, BF), vm((NY, CHUNKS, S, CHUNK, 2 * B), BF),
        vm((4,) + slab, BF), vm((NY, 2) + slab, BF), vm((2, NY, 2) + slab, BF),
        vm((NY, 2, CHUNKS, S, CHUNK, 2 * B), BF), vm((H, ROWS, 2 * S * E), BF), vm((H, ROWS, 4 * S * E), BF),
        vm((H, NX, ROWS // NX, HALF), BF), vm((H, NX - 1, ROWS // NX, HALF), BF),
        vm((H, NZ, SHARE, HALF), BF), vm((H, NZ - 1, SHARE, HALF), BF), vm((H, NX, NZ, SHARE, HALF), BF),
        vm((2, H, NX, ROWS // NX, QUARTER), BF), vm((2, H, NX - 1, ROWS // NX, QUARTER), BF),
        vm((2, H, NZ, SHARE, QUARTER), BF), vm((2, H, NZ - 1, SHARE, QUARTER), BF),
        vm((2, H, NX, NZ, SHARE, QUARTER), BF),
        vm((NZ, SHARE, B), F32), vm((NX, SHARE, B), F32), vm((2, 2, H, S, E, B), BF), vm((NY, H, S, E, B), BF),
        dma((5,)), dma, dma((CHUNKS,)), dma, dma, dma, dma((NY - 1,)), dma, dma((2, NY - 1)), dma, dma((2, NY - 1)),
        dma, dma, dma, dma((2,)), dma, dma((2,)),
        dma((2,)), dma((3, H)), dma((2,)), dma((3, H)), dma((2,)), dma((3, H)), dma((2,)), dma((3, H)), dma((H,)),
        dma, dma, dma, dma, dma, dma,
    ]
    anywhere = pl.BlockSpec(memory_space=pl.ANY)
    vmem = pl.BlockSpec(memory_space=pltpu.VMEM)
    attended = pl.pallas_call(
        kernel,
        out_shape=jax.ShapeDtypeStruct((S, B, D), BF),
        in_specs=[anywhere] * 5,
        out_specs=vmem,
        scratch_shapes=scratch,
        compiler_params=pltpu.CompilerParams(
            collective_id=0, has_side_effects=True, vmem_limit_bytes=56 * 1024 * 1024
        ),
        name="tied_row_attention",
    )(rows, gain, wq, wk, wv)
    mixed = jnp.dot(attended.reshape(S * B, D), wf, preferred_element_type=F32).astype(BF)
    return mixed.reshape(S, B, D)


def solution(mesh):
    placed = (P("seq", "res", None), P(), P(), P(), P(), P())
    return jax.shard_map(
        body, mesh=mesh, in_specs=placed, out_specs=P("seq", "res", None), check_vma=False
    )
```

```python
import jax
import jax.numpy as jnp
from jax import lax
from jax.experimental import pallas as pl
from jax.experimental.pallas import tpu as pltpu
from jax.sharding import PartitionSpec as P

MESH = pl.DeviceIdType.MESH
BF = jnp.bfloat16
F32 = jnp.float32
NX, NY, NZ = 4, 4, 4
S, B, D = 3, 128, 768
H, E = 3, 64
ROWS = 256
HALF = NY * B
QUARTER = HALF // 2
CHUNKS, CHUNK = 4, B // 4
SHARE = ROWS // NX // NZ


def kernel(
    x_hbm, gain_hbm, wq_hbm, wk_hbm, wv_hbm, out_ref,
    xo, gain_ref, xp, xn, wq, wk, wv, wide, qt, kt, vt, kn, qr, kr, vr, kf, qn, qz,
    xs, xr, zs, zr, pf, xsf, xrf, zsf, zrf, pff, fz, ff, os, orr,
    lsem, zss, zrs, qss, qrs, kss, krs, vss, vrs, nss, nrs, kfs, kfr, vfs, vfr, nfs, nfr,
    xss, xrs, lss, lrs, pzs, pzr, pxs, pxr, pnr, fzs, fzr, fxs, fxr, oss, osr,
):
    seq, res = lax.axis_index("seq"), lax.axis_index("res")
    c, x, zl = lax.rem(seq, 2), lax.rem(seq // 2, NX), seq // (2 * NX)
    y, zh = lax.rem(res, NY), res // NY

    def dev(x=x, zl=zl, c=c, y=y, zh=zh):
        return ((zl * NX + x) * 2 + c, zh * NY + y)

    def up(i, d, n):
        return lax.rem(i + d, n)

    other = dev(c=1 - c)

    def send(src, dst, ss, rs, to):
        return pltpu.make_async_remote_copy(
            src_ref=src, dst_ref=dst, send_sem=ss, recv_sem=rs, device_id=to, device_id_type=MESH
        )

    barrier = pltpu.get_barrier_semaphore()
    peers = [other, dev(zh=1 - zh)]
    peers += [dev(x=up(x, d, NX)) for d in range(1, NX)]
    peers += [dev(zl=up(zl, d, NZ)) for d in range(1, NZ)]
    peers += [dev(y=up(y, d, NY), c=k) for d in range(1, NY) for k in range(2)]
    for peer in peers:
        pl.semaphore_signal(barrier, inc=1, device_id=peer, device_id_type=MESH)
    loads = [
        pltpu.make_async_copy(a, b, lsem.at[i])
        for i, (a, b) in enumerate(((x_hbm, xo), (gain_hbm, gain_ref), (wq_hbm, wq), (wk_hbm, wk), (wv_hbm, wv)))
    ]
    for copy in loads:
        copy.start()

    pl.semaphore_wait(barrier, len(peers))

    loads[0].wait()

    def landed(ref, rs):
        send(ref, ref, rs, rs, other).wait_recv()

    def left(ref, ss):
        send(ref, ref, ss, ss, other).wait_send()

    def rows_over(q):
        rows = pl.ds(q * CHUNK, CHUNK)
        return send(xo.at[:, rows], xp.at[:, rows], zss, zrs.at[q], dev(zh=1 - zh))

    for q in range(CHUNKS):
        rows_over(q).start()

    def norm(rows):
        rows = rows.astype(F32)
        center = rows - jnp.mean(rows, axis=-1, keepdims=True)
        spread = jnp.mean(center * center, axis=-1, keepdims=True)
        return (center * lax.rsqrt(spread + 1e-05) * gain_ref[...].reshape(1, D)).astype(BF)

    def project(normed, w):
        out = jnp.dot(normed, w[...], preferred_element_type=F32).astype(BF)
        return out.T.reshape(NY, H, E, B)

    def q_copy(s, d):
        b = (-d) % NY
        to = dev(y=up(y, d, NY), c=b // 2)
        return send(qt.at[up(y, d, NY), s], qr.at[b % 2 * 2 + c, s], qss, qrs, to)

    def k_copy(s, d):
        g = up(y, d, NY)
        return send(kt.at[g, s], kr.at[(-d) % NY, c, s], kss, krs.at[d - 1], dev(y=g))

    def v_copy(half, s, d):
        g = up(y, d, NY)
        return send(vt.at[half, g, s], vr.at[half, (-d) % NY, c, s], vss, vrs.at[half, d - 1], dev(y=g))

    def far_copy(q, d):
        g = up(y, d, NY)
        return send(kn.at[g, q], kf.at[(-d) % NY, c, q], nss, nrs.at[q // 2, d - 1], dev(y=g))

    def pair(q):
        return pl.ds(2 * q, 2)

    def k_forward(rel):
        part = kr.at[rel, c]
        return send(part, part, kfs, kfr, other)

    def v_forward(half, rel):
        part = vr.at[half, rel, c]
        return send(part, part, vfs, vfr.at[half], other)

    def far_forward(q, rel):
        part = kf.at[rel, c, pair(q)]
        return send(part, part, nfs, nfr.at[q], other)

    for copy in loads[1:4]:
        copy.wait()

    @pl.loop(0, S)
    def _(s):
        normed = norm(xo[s])
        xn[0, s] = normed
        qt[:, s] = project(normed, wq)
        kt[:, s] = project(normed, wk)
        for d in range(1, NY):
            q_copy(s, d).start()

        @pl.when(c == 1)
        def _():
            q_copy(s, 0).start()

        @pl.when(c == 0)
        def _():
            qr[0, s] = qt[y, s]

        for d in range(1, NY):
            k_copy(s, d).start()
        kr[0, c, s] = kt[y, s]

    k_forward(0).start()
    loads[4].wait()

    for g in range(NY):
        wide[:, g * 2 * B : g * 2 * B + H * E] = wk[:, g * H * E : (g + 1) * H * E]
        wide[:, g * 2 * B + H * E : (g + 1) * 2 * B] = jnp.zeros((D, 2 * B - H * E), BF)

    def values(half):
        @pl.loop(0, S)
        def _(s):
            vt[half, :, s] = project(xn[half, s], wv)
            vr[half, 0, c, s] = vt[half, y, s]

        v_forward(half, 0).start()

    values(0)

    def partner(q):
        rows_over(q).wait_recv()
        normed = norm(xp[:, q * CHUNK : (q + 1) * CHUNK].reshape(S * CHUNK, D))
        xn[1, :, q * CHUNK : (q + 1) * CHUNK] = normed.reshape(S, CHUNK, D)
        keys = jnp.dot(normed, wide[...], preferred_element_type=F32).astype(BF).reshape(S, CHUNK, NY * 2 * B)
        for g in range(NY):
            kn[g, q] = keys[:, :, g * 2 * B : (g + 1) * 2 * B]
        for d in range(1, NY):
            far_copy(q, d).start()
        kf[0, c, q] = kn[y, q]

    def columns(r, h):
        return jnp.concatenate([r[rel, :, :, h].reshape(2 * S * E, B) for rel in range(NY)], axis=1)

    def key_rows(part, tile):
        lanes = pl.ds(tile * B, B)
        return jnp.concatenate(
            [
                jnp.concatenate(
                    [kf[rel, i, pair(part), s, :, lanes].reshape(2 * CHUNK, B) for rel in range(NY)], axis=0
                )
                for i in range(2)
                for s in range(S)
            ],
            axis=1,
        )

    def piece(near, far, p):
        return far.at[p - 1] if p else near

    def x_copy(p, h, d):
        g = up(x, d, NX)
        return send(
            piece(xs, xsf, p).at[h, g], piece(xr, xrf, p).at[h, d - 1], xss.at[min(p, 1)], xrs.at[p, h], dev(x=g)
        )

    above, below = up(x, 1, NX), up(x, 3, NX)

    def gather_first(h):
        part = pf.at[h, x]
        return [send(part, part, pxs.at[0], pnr.at[h], dev(x=to)) for to in (above, below)]

    def gather_second(h):
        landed(pf.at[h, pl.ds(0, 2)], pnr.at[h])
        for source, to, first in ((below, above, 0), (above, below, 2)):
            part = pf.at[h, source, pl.ds(first, 2)]
            send(part, part, pxs.at[0], pxr.at[0, h], dev(x=to)).start()

    def z_copy(p, h, d):
        g = up(zl, d, NZ)
        return send(
            piece(zs, zsf, p).at[h, g], piece(zr, zrf, p).at[h, d - 1], lss.at[min(p, 1)], lrs.at[p, h], dev(zl=g)
        )

    def pz_copy(p, h, d):
        part = piece(pf, pff, p).at[h, x, zl]
        return send(part, part, pzs.at[min(p, 1)], pzr.at[p, h], dev(zl=up(zl, d, NZ)))

    def px_copy(p, h, d):
        part = piece(pf, pff, p).at[h, x]
        return send(part, part, pxs.at[min(p, 1)], pxr.at[p, h], dev(x=up(x, d, NX)))

    def fz_copy(d):
        part = fz.at[zl]
        return send(part, part, fzs, fzr, dev(zl=up(zl, d, NZ)))

    def fx_copy(d):
        part = ff.at[x]
        return send(part, part, fxs, fxr, dev(x=up(x, d, NX)))

    def logits(p):
        if p:
            landed(kf.at[:, c, pair(p - 1)], nfr.at[p - 1])
            rows = [key_rows(p - 1, tile) for tile in range(2)]
        else:
            landed(kr.at[:, c], kfr)
        for h in range(H):
            if p:
                part = lax.dot_general(
                    qz[h], rows[h // 2], (((1,), (1,)), ((), ())), preferred_element_type=F32
                ).astype(BF)
                xsf[p - 1, h] = part.reshape(NX, ROWS // NX, QUARTER)
            else:
                part = jnp.dot(qn[h], columns(kr, h), preferred_element_type=F32).astype(BF)
                xs[h] = part.reshape(NX, ROWS // NX, HALF)
            for d in range(1, NX):
                x_copy(p, h, d).start()

    def over_x(p, h):
        mine, theirs, into = piece(xs, xsf, p), piece(xr, xrf, p), piece(zs, zsf, p)
        landed(theirs.at[h], xrs.at[p, h])
        total = mine[h, x].astype(F32)
        for d in range(1, NX):
            total += theirs[h, d - 1].astype(F32)
        into[h] = total.astype(BF).reshape(NZ, SHARE, total.shape[-1])
        for d in range(1, NZ):
            z_copy(p, h, d).start()

    scale = 1.0 / (8.0 * (96.0**0.5))
    tops, sums = [[], []], [[], []]
    lane = lax.broadcasted_iota(jnp.int32, (SHARE, B), 1)
    factors = [jnp.zeros((SHARE, B), F32)]

    def softmax(p, h):
        mine, theirs = piece(zs, zsf, p), piece(zr, zrf, p)
        landed(theirs.at[h], lrs.at[p, h])
        total = mine[h, zl].astype(F32)
        for d in range(1, NZ):
            total += theirs[h, d - 1].astype(F32)
        top = jnp.max(total, axis=-1, keepdims=True)
        if p:
            top = jnp.maximum(top, tops[p - 1][h])
        weights = jnp.exp((total - top) * scale)
        whole = jnp.sum(weights, axis=-1, keepdims=True)
        if p < 2:
            tops[p].append(top)
            sums[p].append(whole)
        else:
            old = [jnp.exp((tops[i][h] - top) * scale) for i in range(2)]
            inverse = 1.0 / (old[0] * sums[0][h] + old[1] * sums[1][h] + whole)
            weights *= inverse
            for i in range(2):
                factors[0] = jnp.where(lane == 4 * i + h, old[i] * inverse, factors[0])
        piece(pf, pff, p)[h, x, zl] = weights.astype(BF)
        for d in range(1, NZ):
            pz_copy(p, h, d).start()

    def pass_on(p, h):
        landed(piece(pf, pff, p).at[h, x, pl.ds(0, NZ - 1)], pzr.at[p, h])
        for copy in [px_copy(p, h, d) for d in range(1, NX)] if p else gather_first(h):
            copy.start()

    def share_keys(part):
        for d in range(1, NY):
            landed(kf.at[(-d) % NY, c, pair(part)], nrs.at[part, d - 1])
            far_forward(part, (-d) % NY).start()

    def share_values(half):
        for d in range(1, NY):
            landed(vr.at[half, (-d) % NY, c], vrs.at[half, d - 1])
            v_forward(half, (-d) % NY).start()

    def send_values(half, s):
        for d in range(1, NY):
            v_copy(half, s, d).start()

    partner(0)
    for s in range(S):
        send_values(0, s)
    for d in range(1, NY):
        landed(kr.at[(-d) % NY, c], krs.at[d - 1])
        k_forward((-d) % NY).start()
    @pl.when(c == 0)
    def _():
        landed(qr.at[pl.ds(1, 3)], qrs)

    @pl.when(c == 1)
    def _():
        landed(qr, qrs)

    @pl.loop(0, H)
    def _(h):
        cols = [qr[2 * b : 2 * b + 2, :, h].reshape(2 * S * E, B).T for b in range(2)]
        qn[h] = jnp.concatenate(cols, axis=0)

    logits(0)
    partner(1)
    far_forward(0, 0).start()
    none = jnp.zeros((E, ROWS), BF)
    for h in range(H):
        rows = []
        for i in range(2):
            for s in range(S):
                query = jnp.concatenate([qr[2 * b + i, s, h] for b in range(2)], axis=1)
                rows += [none, query] if h == 1 else [query, none]
        qz[h] = jnp.concatenate(rows, axis=0).T

    partner(2)
    share_keys(0)
    over_x(0, 0)
    logits(1)
    over_x(0, 1)
    over_x(0, 2)
    partner(3)
    far_forward(1, 0).start()
    values(1)
    over_x(1, 0)
    over_x(1, 1)
    over_x(1, 2)
    share_keys(1)
    softmax(0, 0)
    softmax(0, 1)
    softmax(0, 2)
    logits(2)
    for s in range(S):
        send_values(1, s)
    softmax(1, 0)
    softmax(1, 1)
    softmax(1, 2)
    over_x(2, 0)
    pass_on(0, 0)
    pass_on(0, 1)
    pass_on(0, 2)
    over_x(2, 1)
    over_x(2, 2)
    softmax(2, 0)
    pass_on(1, 0)
    softmax(2, 1)
    gather_second(0)
    softmax(2, 2)
    fz[zl] = factors[0]
    for d in range(1, NZ):
        fz_copy(d).start()
    gather_second(1)
    gather_second(2)
    share_values(0)
    share_values(1)
    pass_on(2, 0)
    pass_on(1, 1)
    landed(fz.at[pl.ds(0, NZ - 1)], fzr)
    packed = fz[0]
    for k in range(1, NZ):
        packed = jnp.where((lane >= 8 * k) & (lane < 8 * k + 8), pltpu.roll(fz[k], 8 * k, 1), packed)
    ff[x] = packed
    for d in range(1, NX):
        fx_copy(d).start()
    pass_on(2, 1)
    pass_on(1, 2)
    pass_on(2, 2)
    for half in range(2):
        landed(vr.at[half, :, c], vfr.at[half])

    def o_copy(slot, k, h):
        b = 2 * c + slot
        return send(os.at[slot, k, h], orr.at[y, h], oss, osr, dev(y=up(y, b, NY), c=k))

    landed(ff.at[pl.ds(0, NX - 1)], fxr)
    for h in range(H):
        own = [
            jnp.concatenate(
                [ff[i, :, 8 * k + 4 * n + h : 8 * k + 4 * n + h + 1] for i in range(NX) for k in range(NZ)], axis=0
            )
            for n in range(2)
        ]
        landed(pf.at[h, 0], pxr.at[0, h])
        near = (pf[h].reshape(ROWS, HALF).astype(F32) * own[0]).astype(BF)
        total = lax.dot_general(
            columns(vr.at[0], h), near, (((1,), (1,)), ((), ())), preferred_element_type=F32
        )
        landed(pff.at[0, h, pl.ds(0, NX - 1)], pxr.at[1, h])
        first = pff[0, h].reshape(ROWS, QUARTER).astype(F32) * own[1]
        landed(pff.at[1, h, pl.ds(0, NX - 1)], pxr.at[2, h])
        second = pff[1, h].reshape(ROWS, QUARTER).astype(F32)
        low = lax.broadcasted_iota(jnp.int32, (ROWS, B), 1) < B // 2
        far = []
        for k in range(2):
            one, two = first[:, k * B : (k + 1) * B], second[:, k * B : (k + 1) * B]
            far.append(jnp.where(low, one, pltpu.roll(two, B // 2, 1)))
            far.append(jnp.where(low, pltpu.roll(one, B // 2, 1), two))
        total += lax.dot_general(
            columns(vr.at[1], h),
            jnp.concatenate(far, axis=1).astype(BF),
            (((1,), (1,)), ((), ())),
            preferred_element_type=F32,
        )
        total = total.astype(BF)
        for b in range(2):
            os[b, :, h] = total[:, b * B : (b + 1) * B].reshape(2, S, E, B)
        for slot, k in ((1, 0), (1, 1), (0, 1)):
            o_copy(slot, k, h).start()

        @pl.when(c == 1)
        def _():
            o_copy(0, 0, h).start()

        @pl.when(c == 0)
        def _():
            orr[y, h] = os[0, 0, h]

    @pl.when(c == 0)
    def _():
        landed(orr.at[pl.ds(1, 3)], osr)

    @pl.when(c == 1)
    def _():
        landed(orr, osr)

    @pl.loop(0, S)
    def _(s):
        out_ref[s] = orr[:, :, s].reshape(D, B).T

    left(xo, zss)
    left(kt.at[pl.ds(1, NY - 1)], kss)
    left(vt.at[:, pl.ds(1, NY - 1)], vss)
    left(kn.at[pl.ds(1, NY - 1)], nss)
    left(kr.at[:, c], kfs)
    left(vr.at[:, :, c], vfs)
    left(kf.at[:, c], nfs)
    left(xs.at[:, pl.ds(1, NX - 1)], xss.at[0])
    left(xsf.at[:, :, pl.ds(1, NX - 1)], xss.at[1])
    left(zs.at[:, pl.ds(1, NZ - 1)], lss.at[0])
    left(zsf.at[:, :, pl.ds(1, NZ - 1)], lss.at[1])
    left(pf.at[:, 0, pl.ds(1, NZ - 1)], pzs.at[0])
    left(pff.at[:, :, 0, pl.ds(1, NZ - 1)], pzs.at[1])
    left(pf.at[:, pl.ds(1, NX - 1)], pxs.at[0])
    left(pff.at[:, :, pl.ds(1, NX - 1)], pxs.at[1])
    left(fz.at[pl.ds(1, NZ - 1)], fzs)
    left(ff.at[pl.ds(1, NX - 1)], fxs)

    @pl.when(c == 0)
    def _():
        left(qt.at[pl.ds(1, 3)], qss)
        left(orr.at[pl.ds(1, 3)], oss)

    @pl.when(c == 1)
    def _():
        left(qt, qss)
        left(orr, oss)


def body(rows, gain, wq, wk, wv, wf):
    slab = (S, H, E, B)
    dma, vm = pltpu.SemaphoreType.DMA, pltpu.VMEM
    scratch = [
        vm((S, B, D), BF), vm((D,), F32), vm((S, B, D), BF), vm((2, S, B, D), BF),
        vm((D, D), BF), vm((D, D), BF), vm((D, D), BF), vm((D, NY * 2 * B), BF),
        vm((NY,) + slab, BF), vm((NY,) + slab, BF), vm((2, NY) + slab, BF), vm((NY, CHUNKS, S, CHUNK, 2 * B), BF),
        vm((4,) + slab, BF), vm((NY, 2) + slab, BF), vm((2, NY, 2) + slab, BF),
        vm((NY, 2, CHUNKS, S, CHUNK, 2 * B), BF), vm((H, ROWS, 2 * S * E), BF), vm((H, ROWS, 4 * S * E), BF),
        vm((H, NX, ROWS // NX, HALF), BF), vm((H, NX - 1, ROWS // NX, HALF), BF),
        vm((H, NZ, SHARE, HALF), BF), vm((H, NZ - 1, SHARE, HALF), BF), vm((H, NX, NZ, SHARE, HALF), BF),
        vm((2, H, NX, ROWS // NX, QUARTER), BF), vm((2, H, NX - 1, ROWS // NX, QUARTER), BF),
        vm((2, H, NZ, SHARE, QUARTER), BF), vm((2, H, NZ - 1, SHARE, QUARTER), BF),
        vm((2, H, NX, NZ, SHARE, QUARTER), BF),
        vm((NZ, SHARE, B), F32), vm((NX, SHARE, B), F32), vm((2, 2, H, S, E, B), BF), vm((NY, H, S, E, B), BF),
        dma((5,)), dma, dma((CHUNKS,)), dma, dma, dma, dma((NY - 1,)), dma, dma((2, NY - 1)), dma, dma((2, NY - 1)),
        dma, dma, dma, dma((2,)), dma, dma((2,)),
        dma((2,)), dma((3, H)), dma((2,)), dma((3, H)), dma((2,)), dma((3, H)), dma((2,)), dma((3, H)), dma((H,)),
        dma, dma, dma, dma, dma, dma,
    ]
    anywhere = pl.BlockSpec(memory_space=pl.ANY)
    vmem = pl.BlockSpec(memory_space=pltpu.VMEM)
    attended = pl.pallas_call(
        kernel,
        out_shape=jax.ShapeDtypeStruct((S, B, D), BF),
        in_specs=[anywhere] * 5,
        out_specs=vmem,
        scratch_shapes=scratch,
        compiler_params=pltpu.CompilerParams(
            collective_id=0, has_side_effects=True, vmem_limit_bytes=53 * 1024 * 1024
        ),
        name="tied_row_attention",
    )(rows, gain, wq, wk, wv)
    mixed = jnp.dot(attended.reshape(S * B, D), wf, preferred_element_type=F32).astype(BF)
    return mixed.reshape(S, B, D)


def solution(mesh):
    placed = (P("seq", "res", None), P(), P(), P(), P(), P())
    return jax.shard_map(
        body, mesh=mesh, in_specs=placed, out_specs=P("seq", "res", None), check_vma=False
    )
```
